512 devices in a mesh: tile: 64 (over y, z_hi, x), tm: 8 (over z_lo, core).
Axes of the slice: x: 4, y: 8, z: 8 (z_hi: 2, z_lo: 4; z = z_hi * 4 + z_lo), core: 2. Of those that a mesh axis runs over, the one named last changes fastest.
Arguments:
- latent: bfloat16 [16, 64, 1, 5, 16], P('tm', 'tile'), may hold values from -33 to 33
- proj_weight: bfloat16 [16, 256], replicated, may hold values from -1.5 to 1.5
- first_gain: float32 [256], replicated, may hold values from 0.1 to 1.9
- first_shift: float32 [256], replicated, may hold values from -0.5 to 0.5
- half_weight: bfloat16 [27, 256, 256], replicated, may hold values from -0.078125 to 0.078125
- second_gain: float32 [256], replicated, may hold values from 0.1 to 1.9
- second_shift: float32 [256], replicated, may hold values from -0.5 to 0.5
- full_weight: bfloat16 [27, 256, 128], P(None, None, 'tm'), may hold values from -0.078125 to 0.078125
- full_bias: float32 [128], replicated, may hold values from -0.5 to 0.5
- anchors: int32 [65], replicated, may hold values from 0 to 320, as said below
- reach: int32 [65], replicated, may hold values from 0 to 4, as said below
Outputs:
- decoded: bfloat16 [16, 64, 8, 40, 128], P('tm', 'tile')
The draws below stay inside these ranges and needn't reach their ends.
Inputs may be any that keep to these rules, and one draw needn't show every extreme that they name: `anchors`: entry 0 is 0 and entry 64 is 320; entry j differs from j * 5 by at most 1, and both extremes occur in every draw. `reach`: entries 0 and 64 are 0; the others are 1 to 4; entry 1 is 4, and 1 occurs in every draw.
All inputs are finite; a program needn't handle non-finite values.
Results may differ from the reference program's by a relative error of at most 0.0055.
Values may be sent and summed in bfloat16 or wider, within the bound.
A program may use at most 64 MiB of HBM per device.

```python
import jax
import jax.numpy as jnp
from jax import lax

LAT = 16
CH_HALF = 256
CH_FULL = 128
GROUPS = 32
FR = 2
LCW = 5
SHIFT = 1
EXT = 4
LH = 1
CTILES = 64
MARGIN = 5
BUF = 15
FRAMES = 16
LW = 320
N_TM = 8


def draw_latent(key, part):
    noise_key, rough_key = jax.random.split(jax.random.fold_in(key, 3), 2)
    columns = jnp.arange(LW, dtype=jnp.float32)
    column_ramp = (1.0 + 2.0 * columns / max(LW - 1, 1))[None, None, :, None]
    rough = jax.random.uniform(rough_key, (1, 1, LW, LAT), jnp.float32, 0.6, 1.8)
    base_draw = jnp.clip(jax.random.normal(noise_key, (FRAMES, LH, LW, LAT), jnp.float32), -6.0, 6.0)
    values = base_draw * rough * column_ramp
    tiled = values.reshape(FRAMES, LH, CTILES, LCW, LAT).transpose(0, 2, 1, 3, 4)
    return tiled.astype(jnp.bfloat16)


def draw_anchors(key, part):
    shift_key, place_key = jax.random.split(jax.random.fold_in(key, 11))
    shifts = jax.random.randint(shift_key, (CTILES + 1,), -SHIFT, SHIFT + 1)
    chosen = jax.random.randint(place_key, (), 1, CTILES)
    partner = 1 + chosen % (CTILES - 1)
    shifts = shifts.at[chosen].set(SHIFT).at[partner].set(-SHIFT)
    places = jnp.arange(CTILES + 1, dtype=jnp.int32)
    shifts = jnp.where((places == 0) | (places == CTILES), 0, shifts)
    return (places * LCW + shifts).astype(jnp.int32)


def draw_reach(key, part):
    reach_key, place_key = jax.random.split(jax.random.fold_in(key, 17))
    extents = jax.random.randint(reach_key, (CTILES + 1,), 1, EXT + 1)
    chosen = jax.random.randint(place_key, (), 2, CTILES)
    extents = extents.at[1].set(EXT).at[chosen].set(1)
    places = jnp.arange(CTILES + 1, dtype=jnp.int32)
    extents = jnp.where((places == 0) | (places == CTILES), 0, extents)
    return extents.astype(jnp.int32)


def block_scale(rng, extent, cuts, least, top_value):
    loudness, own = 1.0, jax.random.fold_in(rng, 6)
    for position, blocks in cuts:
        steps = jnp.exp(jax.random.uniform(jax.random.fold_in(own, position), (blocks,), jnp.float32, least / len(cuts), top_value / len(cuts)))
        loudness = loudness * jnp.repeat(steps, extent[position] // blocks).reshape([-1 if axis == position else 1 for axis in range(len(extent))])
    return loudness


def gaussian(key, extent, scale, most, pieces=(), held_as=jnp.bfloat16):
    values = jax.random.normal(key, extent, jnp.float32) * scale
    if len(pieces) > 0:
        values = block_scale(key, extent, pieces, -0.22, 0.18) * values
    return jnp.clip(values, min=-most, max=most).astype(held_as)


def setup_inputs(seed: int = 0) -> dict:
    keys = jax.random.split(jax.random.key(seed), 12)
    return {
        "latent": draw_latent(jax.random.fold_in(keys[11], 71), 0),
        "proj_weight": gaussian(keys[1], (LAT, CH_HALF), LAT ** -0.5, 1.5),
        "first_gain": jnp.clip(1.0 + 0.18 * jax.random.normal(keys[2], (CH_HALF,), jnp.float32), 0.1, 1.9),
        "first_shift": jnp.clip(jax.random.uniform(keys[3], (CH_HALF,), jnp.float32, -0.5, 0.5), -0.5, 0.5),
        "half_weight": gaussian(keys[4], (27, CH_HALF, CH_HALF), (27 * CH_HALF) ** -0.5, 0.078125),
        "second_gain": jnp.clip(1.0 + 0.18 * jax.random.normal(keys[5], (CH_HALF,), jnp.float32), 0.1, 1.9),
        "second_shift": jnp.clip(jax.random.uniform(keys[6], (CH_HALF,), jnp.float32, -0.5, 0.5), -0.5, 0.5),
        "full_weight": gaussian(keys[7], (27, CH_HALF, CH_FULL), (27 * CH_HALF) ** -0.5, 0.078125, ((2, 8),)),
        "full_bias": jnp.clip(jax.random.uniform(keys[8], (CH_FULL,), jnp.float32, -0.5, 0.5), -0.5, 0.5),
        "anchors": draw_anchors(jax.random.fold_in(keys[11], 71), 0),
        "reach": draw_reach(jax.random.fold_in(keys[11], 71), 0),
    }


def convolve(sequence, kernel_rows, row_pad):
    kernel = kernel_rows.reshape(3, 3, 3, kernel_rows.shape[1], kernel_rows.shape[2])
    result = lax.conv_general_dilated(sequence[None], kernel, (1, 1, 1), ((0, 0), (row_pad, row_pad), (1, 1)), dimension_numbers=('NDHWC', 'DHWIO', 'NDHWC'), preferred_element_type=jnp.float32)
    return result[0]

def enlarge(values, factor):
    return jnp.repeat(jnp.repeat(values, factor, axis=1), factor, axis=2)

def moments(sums, squares, count):
    mean_value = sums / count
    variance = squares / count - mean_value * mean_value
    return (mean_value, lax.rsqrt(variance + 1e-06))

def normalize(values, mean_value, scale_value, gain, shift):
    return jax.nn.silu(gain * (values - mean_value) * scale_value + shift)

def blend_weight(tile_id, columns, anchors, reach):
    left_edge = 8 * anchors[tile_id]
    right_edge = 8 * anchors[tile_id + 1]
    left_reach = 8 * reach[tile_id]
    right_reach = 8 * reach[tile_id + 1]
    place = columns.astype(jnp.float32)
    rising = jnp.clip((place - (left_edge - left_reach).astype(jnp.float32) + 0.5) / jnp.maximum(2 * left_reach, 1).astype(jnp.float32), 0.0, 1.0)
    rising = jnp.where(left_reach > 0, rising, jnp.where(columns >= left_edge, 1.0, 0.0))
    falling = jnp.clip(((right_edge + right_reach).astype(jnp.float32) - place - 0.5) / jnp.maximum(2 * right_reach, 1).astype(jnp.float32), 0.0, 1.0)
    falling = jnp.where(right_reach > 0, falling, jnp.where(columns < right_edge, 1.0, 0.0))
    return jnp.minimum(rising, falling).astype(jnp.float32)

def per_frame(values, group_width):
    return jnp.repeat(jnp.repeat(values, group_width, axis=1), FR, axis=0)[:, None, None, :]

def reference(latent, proj_weight, first_gain, first_shift, half_weight, second_gain, second_shift, full_weight, full_bias, anchors, reach):
    channels = CH_HALF
    group_width = CH_HALF // GROUPS
    frame_latent = latent.transpose(0, 2, 1, 3, 4).reshape(FRAMES, LH, LW, LAT)
    projected = jnp.dot(frame_latent.reshape(-1, LAT), proj_weight, preferred_element_type=jnp.float32).reshape(FRAMES, LH, LW, channels)
    blocked = projected.reshape(N_TM, FR * LH * LW, GROUPS, group_width)
    first_mean, first_scale = moments(lax.optimization_barrier(jnp.sum(blocked, axis=(1, 3))), lax.optimization_barrier(jnp.sum(blocked * blocked, axis=(1, 3))), FR * LH * LW * group_width)
    first_act = normalize(projected, per_frame(first_mean, group_width), per_frame(first_scale, group_width), first_gain, first_shift).astype(jnp.bfloat16)
    padded = jnp.pad(first_act, ((0, 0), (0, 0), (MARGIN, MARGIN), (0, 0)))

    def reach_mask(tile_id, factor, width):
        lower_col = factor * (anchors[tile_id] - reach[tile_id])
        upper_col = factor * (anchors[tile_id + 1] + reach[tile_id + 1])
        places = factor * (tile_id * LCW - MARGIN) + jnp.arange(width, dtype=jnp.int32)
        return (places >= lower_col) & (places < upper_col)

    def half_tile(tile_id):
        window = lax.dynamic_slice_in_dim(padded, (tile_id * LCW).astype(jnp.int32), BUF, 2)
        first_in = jnp.where(reach_mask(tile_id, 1, BUF)[:, None], window, jnp.zeros((), jnp.bfloat16))
        sequence = enlarge(jnp.concatenate([first_in[:1], first_in[:1], first_in], 0), 4)
        middle = convolve(sequence, half_weight, 1)
        places = 4 * (tile_id * LCW - MARGIN) + jnp.arange(4 * BUF, dtype=jnp.int32)
        core_mask = (places >= 4 * anchors[tile_id]) & (places < 4 * anchors[tile_id + 1])
        masked = jnp.where(core_mask[:, None], middle, 0.0).reshape(N_TM, -1, GROUPS, group_width)
        return (middle, lax.optimization_barrier(jnp.sum(masked, axis=(1, 3))), lax.optimization_barrier(jnp.sum(masked * masked, axis=(1, 3))))
    tile_ids = jnp.arange(CTILES, dtype=jnp.int32)
    middles, sums, squares = lax.map(half_tile, tile_ids)
    second_mean, second_scale = moments(lax.optimization_barrier(jnp.sum(sums, axis=0)), lax.optimization_barrier(jnp.sum(squares, axis=0)), FR * 16 * LH * LW * group_width)
    mean_frames = per_frame(second_mean, group_width)
    scale_frames = per_frame(second_scale, group_width)

    def full_tile(inputs):
        tile_id, middle = inputs
        normed = normalize(middle, mean_frames, scale_frames, second_gain, second_shift)
        second_act = jnp.where(reach_mask(tile_id, 4, 4 * BUF)[:, None], normed, 0.0).astype(jnp.bfloat16)
        sequence = enlarge(jnp.concatenate([second_act[:1], second_act[:1], second_act], 0), 2)
        return (convolve(sequence, full_weight, 1) + full_bias).astype(jnp.bfloat16)
    tile_outs = lax.map(full_tile, (tile_ids, middles))

    def add_tile(tile_id, carry):
        numerator, denominator = carry
        places = 8 * (tile_id * LCW - MARGIN) + jnp.arange(8 * BUF, dtype=jnp.int32)
        weight = blend_weight(tile_id, places, anchors, reach)
        start_col = (8 * tile_id * LCW).astype(jnp.int32)
        contrib = tile_outs[tile_id].astype(jnp.float32) * weight[:, None]
        current = lax.dynamic_slice_in_dim(numerator, start_col, 8 * BUF, 2)
        numerator = lax.dynamic_update_slice_in_dim(numerator, current + contrib, start_col, 2)
        below = lax.dynamic_slice_in_dim(denominator, start_col, 8 * BUF, 0)
        denominator = lax.dynamic_update_slice_in_dim(denominator, below + weight, start_col, 0)
        return (numerator, denominator)
    wide_cols = 8 * (LW + 2 * MARGIN)
    numerator, denominator = lax.fori_loop(0, CTILES, add_tile, (jnp.zeros((FRAMES, 8 * LH, wide_cols, CH_FULL), jnp.float32), jnp.zeros((wide_cols,), jnp.float32)))
    inner = numerator[:, :, 8 * MARGIN:8 * MARGIN + 8 * LW]
    weights_sum = denominator[8 * MARGIN:8 * MARGIN + 8 * LW]
    decoded_frame = (inner / weights_sum[:, None]).astype(jnp.bfloat16)
    return decoded_frame.reshape(FRAMES, 8 * LH, CTILES, 8 * LCW, CH_FULL).transpose(0, 2, 1, 3, 4)
```

```python
import jax
import jax.numpy as jnp
from jax import lax
from jax.experimental import pallas as pl
from jax.experimental.pallas import tpu as pltpu
from jax.sharding import PartitionSpec as P

GROUPS = 32
NX, NZH, NY, NT = 4, 2, 8, 8
TILES = NX * NZH * NY
LCW = 5
BF = jnp.bfloat16
F32 = jnp.float32
MESH = pl.DeviceIdType.MESH

COMBOS = ("01", "12", "0", "2", "012")
ROW_USES = {
    "01": ((0, 1), (1, 5), (2, 7)),
    "12": ((0, 0), (1, 2), (2, 6)),
    "0": ((0, 2), (1, 6)),
    "2": ((1, 1), (2, 5)),
    "012": ((1, 3),),
}
COL_USES = {
    "01": ((0, 1, 0), (1, 5, 0), (2, 7, 0)),
    "12": ((0, 0, 0), (1, 2, 0), (2, 6, 0)),
    "0": ((0, 2, 0), (1, 6, 0), (2, 0, 1)),
    "2": ((0, 7, -1), (1, 1, 0), (2, 5, 0)),
    "012": ((1, 3, 0),),
}
SLOT = {0: 0, 1: 1, 2: 2, 3: 3, 4: 3, 5: 4, 6: 5, 7: 6}


def dot(a, b):
    return jnp.dot(a, b, preferred_element_type=F32)


def exact_dot(x, ones):
    high = x.astype(BF)
    rest = x - high.astype(F32)
    middle = rest.astype(BF)
    low = (rest - middle.astype(F32)).astype(BF)
    return dot(high, ones) + dot(middle, ones) + dot(low, ones)


def iota(shape, dim):
    return lax.broadcasted_iota(jnp.int32, shape, dim)


def encode(sums, squares):
    channel, lane = iota((256, 128), 0), iota((256, 128), 1)
    ones = jnp.where(((channel >> 3) == (lane & 31)) & (lane < 64), 1.0, 0.0).astype(BF)
    row = iota((8, 256), 0)
    stacked = jnp.where(row == 0, sums, jnp.where(row == 1, squares, 0.0))
    coded = exact_dot(stacked, ones)
    return jnp.where(iota((1, 128), 1) < 32, coded[0:1], coded[1:2])


def decode(totals, count):
    lane, channel = iota((128, 256), 0), iota((128, 256), 1)
    ones = jnp.where(((channel >> 3) == (lane & 31)) & (lane < 64), 1.0, 0.0).astype(BF)
    row, place = iota((8, 128), 0), iota((8, 128), 1)
    stacked = jnp.zeros((8, 128), F32)
    for i, total in enumerate(totals):
        stacked = jnp.where((row == 2 * i) & (place < 32), total, stacked)
        stacked = jnp.where((row == 2 * i + 1) & (place >= 32), total, stacked)
    wide = exact_dot(stacked, ones)
    result = []
    for i in range(len(totals)):
        mean = wide[2 * i : 2 * i + 1] / count
        variance = wide[2 * i + 1 : 2 * i + 2] / count - mean * mean
        result.append((mean, lax.rsqrt(variance + 1e-06)))
    return result


def normalize(values, mean, scale, gain, shift):
    v = gain * (values - mean) * scale + shift
    half = 0.5 * v
    return half + half * jnp.tanh(half)


def tile_at(y, z, x):
    return y * (NZH * NX) + z * NX + x


def around(j, k):
    other = j + k
    return jnp.clip(other, 0, TILES - 1), (other >= 0) & (other < TILES)


def front_kernel(
    lat_hbm, wp_hbm, gain_hbm, shift_hbm, hw_hbm, fw_hbm, anchors_hbm, reach_hbm,
    mid_ref, moments_ref, wc_ref,
    lbuf, wp, gain, shift, hw, wt, anchors, reach, fl, a1, b1, a2, b2,
    local_sem, sa1, ra1, sb1, rb1, sa2, ra2, sb2, rb2, sl, rl, sw, rw, ss, rs,
):
    j = lax.axis_index("tile")
    tm = lax.axis_index("tm")
    y, z, x = j // (NZH * NX), (j // NX) % NZH, j % NX
    zl = tm // 2

    loads = [
        pltpu.make_async_copy(src, dst, local_sem.at[i])
        for i, (src, dst) in enumerate(
            (
                (lat_hbm, lbuf.at[0, pl.ds(1, LCW)]),
                (wp_hbm, wp),
                (fw_hbm, wt.at[tm]),
                (anchors_hbm, anchors),
                (reach_hbm, reach),
                (gain_hbm, gain),
                (shift_hbm, shift),
                (hw_hbm.at[pl.ds(0, 9)], hw.at[pl.ds(0, 9)]),
                (hw_hbm.at[pl.ds(9, 9)], hw.at[pl.ds(9, 9)]),
                (hw_hbm.at[pl.ds(18, 9)], hw.at[pl.ds(18, 9)]),
            )
        )
    ]
    for load in loads:
        load.start()

    column = [(tile_at((y + d) % NY, z, x), tm) for d in range(NY)]
    plane = [(s, dz, dx) for s in range(3) for dz in range(NZH) for dx in range(NX)][1:]

    def plane_at(sign, s, dz, dx):
        return (
            tile_at(y, (z + dz) % NZH, (x + sign * dx + NX) % NX),
            (tm + sign * s + NT) % NT,
        )

    def chip_at(step):
        far = (zl + step + 4) // 4
        return (tile_at(y, (z + far + 1) % NZH, x), (tm + 2 * step + NT) % NT)

    sibling = (j, tm + 1 - 2 * (tm % 2))
    chips = [chip_at(1), chip_at(-1), chip_at(2), chip_at(-2)]

    barrier = pltpu.get_barrier_semaphore()
    greeted = column[1:] + [plane_at(-1, *p) for p in plane] + chips + [sibling]
    for s in range(3):
        greeted.append(((j + 1) % TILES, (tm - s + NT) % NT))
        greeted.append(((j + TILES - 1) % TILES, (tm - s + NT) % NT))
    for peer in greeted:
        pl.semaphore_signal(barrier, inc=1, device_id=peer, device_id_type=MESH)

    fl[...] = jnp.zeros_like(fl)
    loads[0].wait()
    loads[1].wait()
    for c in range(LCW):
        fl[pl.ds(32 + 1 + c, 2, stride=8), :] = lbuf[0, 1 + c].astype(F32)
    own = dot(fl[32:48].astype(BF), wp[...])
    a1[0] = encode(jnp.sum(own, axis=0, keepdims=True), jnp.sum(own * own, axis=0, keepdims=True))

    pl.semaphore_wait(barrier, len(greeted))

    def send(src, dst, send_sem, recv_sem, peer):
        copy = pltpu.make_async_remote_copy(
            src_ref=src, dst_ref=dst, send_sem=send_sem, recv_sem=recv_sem,
            device_id=peer, device_id_type=MESH,
        )
        copy.start()
        return copy

    def send_column(buf, s_sem, r_sem):
        return [send(buf.at[0], buf.at[d], s_sem.at[d], r_sem.at[d], column[d]) for d in range(1, NY)]

    def send_plane(buf, s_sem, r_sem, shifts):
        copies = []
        for s, dz, dx in plane:
            if s < shifts:
                i = s * 8 + dz * NX + dx
                copies.append(
                    send(buf.at[0], buf.at[i], s_sem.at[i], r_sem.at[i], plane_at(1, s, dz, dx))
                )
        return copies

    sent = []
    first_column = send_column(a1, sa1, ra1)
    lat_copies = []
    for s in range(3):
        for i, (src, dst, tile) in enumerate(
            (
                (lbuf.at[0, LCW], lbuf.at[s, 0], (j + 1) % TILES),
                (lbuf.at[0, 1], lbuf.at[s, LCW + 1], (j + TILES - 1) % TILES),
                (lbuf.at[0, pl.ds(1, LCW)], lbuf.at[s, pl.ds(1, LCW)], j),
            )
        ):
            if i == 2 and s == 0:
                continue
            n = 3 * s + i
            lat_copies.append(send(src, dst, sl.at[n], rl.at[n], (tile, (tm + s) % NT)))
    loads[2].wait()
    sibling_copies = [send(wt.at[tm], wt.at[tm], ss.at[0], rs.at[0], sibling)]

    for copy in first_column:
        copy.wait_recv()
    b1[0] = jnp.sum(a1[...], axis=0)
    first_plane = send_plane(b1, sb1, rb1, 3)

    half = 14
    chip_copies = [
        send(wt.at[tm], wt.at[tm], sw.at[0], rw.at[0], chips[0]),
        send(wt.at[tm], wt.at[tm], sw.at[1], rw.at[1], chips[1]),
        send(wt.at[tm, pl.ds(0, half)], wt.at[tm, pl.ds(0, half)], sw.at[2], rw.at[2], chips[2]),
        send(
            wt.at[tm, pl.ds(half, 27 - half)], wt.at[tm, pl.ds(half, 27 - half)],
            sw.at[3], rw.at[3], chips[3],
        ),
    ]

    for copy in lat_copies:
        copy.wait_recv()
    for s in range(3):
        for c in range(LCW + 2):
            fl[pl.ds(16 * (2 - s) + c, 2, stride=8), :] = lbuf[s, c].astype(F32)
    projected = dot(fl[...].astype(BF), wp[...])
    for load in loads[3:]:
        load.wait()

    for copy in first_plane:
        copy.wait_recv()
    totals = [jnp.sum(b1[8 * s : 8 * s + 8], axis=0) for s in range(3)]
    stats = decode(totals, float(2 * LCW * TILES * 8))
    frames = []
    for s in (2, 1, 0):
        block = normalize(
            projected[16 * (2 - s) : 16 * (2 - s) + 16], stats[s][0], stats[s][1], gain[...], shift[...]
        )
        frames += [block[0:8], block[8:16]]
    frames[2] = jnp.where(tm == 0, frames[4], frames[2])
    frames[3] = jnp.where(tm == 0, frames[4], frames[3])
    frames[0] = jnp.where(tm == 1, frames[2], frames[0])
    frames[1] = jnp.where(tm == 1, frames[2], frames[1])
    seqs = [jnp.concatenate(frames[a : a + 4], axis=0).astype(BF) for a in range(3)]

    col = 5 * j - 1 + (iota((32, 256), 0) & 7)
    local_col = iota((32, 256), 0) & 7
    masks, cores = [], []
    for k in (-1, 0, 1):
        t, there = around(j, k)
        low, high = anchors[t], anchors[t + 1]
        inside = (col >= low - reach[t]) & (col < high + reach[t + 1])
        masks.append(jnp.where(inside, 1.0, 0.0))
        there = jnp.where(there, 1, 0)
        core = (col >= low) & (col < high) & (local_col >= 1) & (local_col <= LCW)
        cores.append(jnp.where(core, there.astype(F32), 0.0))

    taps = [
        [
            dot(seqs[0], hw[3 * b + d]) + dot(seqs[1], hw[9 + 3 * b + d]) + dot(seqs[2], hw[18 + 3 * b + d])
            for d in range(3)
        ]
        for b in range(3)
    ]
    sums = jnp.zeros((8, 256), F32)
    squares = jnp.zeros((8, 256), F32)

    def rolled(v, by):
        return pltpu.roll(v.reshape(4, 8, 256), by % 8, 1).reshape(32, 256)

    for r in range(3):
        if r == 0:
            q = [taps[1][d] + taps[2][d] for d in range(3)]
        elif r == 1:
            q = [taps[0][d] + taps[1][d] + taps[2][d] for d in range(3)]
        else:
            q = [taps[0][d] + taps[1][d] for d in range(3)]
        right = q[1] + q[2]
        left = q[0] + q[1]
        whole = left + q[2]
        for k in range(3):
            m = masks[k]
            kinds = (
                rolled(m * q[0], 1) + m * right,
                m * whole,
                m * left + rolled(m * q[2], -1),
            )
            for p in range(3):
                mid_ref[k * 9 + r * 3 + p] = kinds[p]
                times = (2.0 if r == 1 else 1.0) * (2.0 if p == 1 else 1.0)
                part = cores[k][16:32] * kinds[p][16:32]
                square = part * kinds[p][16:32]
                sums = sums + times * (part[0:8] + part[8:16])
                squares = squares + times * (square[0:8] + square[8:16])
    a2[0] = encode(jnp.sum(sums, axis=0, keepdims=True), jnp.sum(squares, axis=0, keepdims=True))
    second_column = send_column(a2, sa2, ra2)

    for copy in chip_copies:
        copy.wait_recv()
    for i, shard in enumerate(((tm + 2) % NT, (tm + 4) % NT, (tm + 6) % NT)):
        sibling_copies.append(
            send(wt.at[shard], wt.at[shard], ss.at[1 + i], rs.at[1 + i], sibling)
        )

    for copy in second_column:
        copy.wait_recv()
    b2[0] = jnp.sum(a2[...], axis=0)
    second_plane = send_plane(b2, sb2, rb2, 2)

    for copy in sibling_copies:
        copy.wait_recv()

    def combine(i, carry):
        a, n = i // NT, i % NT
        w = [[wt[n, 9 * a + 3 * b + d].astype(F32) for d in range(3)] for b in range(3)]

        def combos(u):
            first = u[0] + u[1]
            return {"0": u[0], "2": u[2], "01": first, "12": u[1] + u[2], "012": first + u[2]}

        by_col = [combos([w[b][d] for b in range(3)]) for d in range(3)]
        for rc, row_class in enumerate(COMBOS):
            both = combos([by_col[d][row_class] for d in range(3)])
            for cc, col_class in enumerate(COMBOS):
                wc_ref[
                    rc,
                    pl.ds(pl.multiple_of(cc * 128 + n * 16, 16), 16),
                    pl.ds(pl.multiple_of(a * 256, 256), 256),
                ] = both[col_class].astype(BF)
        return carry

    lax.fori_loop(0, 3 * NT, combine, 0)

    for copy in second_plane:
        copy.wait_recv()
    totals = [jnp.sum(b2[8 * s : 8 * s + 8], axis=0) for s in range(2)]
    stats = decode(totals, float(2 * 16 * LCW * TILES * 8))
    moments_ref[0:1] = stats[1][0]
    moments_ref[1:2] = stats[1][1]
    moments_ref[2:3] = stats[0][0]
    moments_ref[3:4] = stats[0][1]
    for copy in (
        first_column + lat_copies + first_plane + chip_copies + second_column + sibling_copies + second_plane
    ):
        copy.wait_send()


def blend_weight(columns, low, high, low_reach, high_reach):
    left_edge, right_edge = 8 * low, 8 * high
    left_reach, right_reach = 8 * low_reach, 8 * high_reach
    place = columns.astype(F32)
    rising = jnp.clip(
        (place - (left_edge - left_reach).astype(F32) + 0.5)
        / jnp.maximum(2 * left_reach, 1).astype(F32),
        0.0,
        1.0,
    )
    rising = jnp.where(left_reach > 0, rising, jnp.where(columns >= left_edge, 1.0, 0.0))
    falling = jnp.clip(
        ((right_edge + right_reach).astype(F32) - place - 0.5)
        / jnp.maximum(2 * right_reach, 1).astype(F32),
        0.0,
        1.0,
    )
    falling = jnp.where(right_reach > 0, falling, jnp.where(columns < right_edge, 1.0, 0.0))
    return jnp.minimum(rising, falling)


def back_kernel(
    mid, moments, wc, gain, shift, bias, anchors, reach, out_ref, xs, acc, rows
):
    j = lax.axis_index("tile")
    tm = lax.axis_index("tm")
    col = 5 * j - 1 + (iota((16, 256), 0) & 7)
    for k in range(3):
        t, _ = around(j, k - 1)
        inside = (col >= anchors[t] - reach[t]) & (col < anchors[t + 1] + reach[t + 1])
        for r in range(3):
            for p in range(3):
                values = mid[k * 9 + r * 3 + p]
                before = normalize(values[0:16], moments[0:1], moments[1:2], gain[...], shift[...])
                now = normalize(values[16:32], moments[2:3], moments[3:4], gain[...], shift[...])
                now = jnp.where(inside, now, 0.0)
                before = jnp.where(inside, before, 0.0)
                first = jnp.concatenate([now[0:8], now[0:8]], axis=0)
                before = jnp.where(tm == 0, first, before)
                at = (r * 3 + p) * 48 + k * 16
                xs[at : at + 16, 0:256] = before.astype(BF)
                xs[at : at + 16, 256:512] = jnp.concatenate([before[8:16], now[0:8]], axis=0).astype(BF)
                xs[at : at + 16, 512:768] = now.astype(BF)

    seen = set()
    for rc, row_class in enumerate(COMBOS):
        uses = ROW_USES[row_class]
        r0, r1 = uses[0][0], uses[-1][0] + 1
        for pair in ((0, 1), (2, 3), (4,)):
            if pair == (4,):
                lhs = [xs[r * 144 + 48 : r * 144 + 96] for r in range(r0, r1)]
                lhs = lhs[0] if len(lhs) == 1 else jnp.concatenate(lhs, axis=0)
                inputs = (1,)
            else:
                lhs = xs[r0 * 144 : r1 * 144]
                inputs = (0, 1, 2)
            rhs = wc[rc, pair[0] * 128 : (pair[-1] + 1) * 128]
            result = lax.dot_general(
                lhs, rhs, (((1,), (1,)), ((), ())), preferred_element_type=F32
            )
            for r, big_row in uses:
                for half, cc in enumerate(pair):
                    for p, big_col, by in COL_USES[COMBOS[cc]]:
                        at = ((r - r0) * len(inputs) + inputs.index(p)) * 48
                        part = result[at : at + 48, half * 128 : half * 128 + 128]
                        if by:
                            part = pltpu.roll(part.reshape(6, 8, 128), by % 8, 1).reshape(48, 128)
                        slot = SLOT[big_row] * 7 + SLOT[big_col]
                        if slot in seen:
                            acc[slot] += part
                        else:
                            seen.add(slot)
                            acc[slot] = part

    weights = []
    for c in range(8):
        columns = 40 * j - 8 + 8 * iota((8, 128), 0) + c
        parts = []
        for k in range(3):
            t, there = around(j, k - 1)
            weight = blend_weight(columns, anchors[t], anchors[t + 1], reach[t], reach[t + 1])
            parts.append(weight * jnp.where(there, 1, 0).astype(F32))
        total = parts[0] + parts[1] + parts[2]
        keep = (iota((8, 128), 0) >= 1) & (iota((8, 128), 0) <= LCW)
        total = jnp.where(keep, total, 1.0)
        weights.append([part / total for part in parts])

    for t in range(2):
        for big_row in (0, 1, 2, 3, 5, 6, 7):
            for c in range(8):
                slot = SLOT[big_row] * 7 + SLOT[c]
                value = None
                for k in range(3):
                    at = k * 16 + t * 8
                    piece = (acc[slot, at : at + 8] + bias[...]).astype(BF).astype(F32) * weights[c][k]
                    value = piece if value is None else value + piece
                rows[pl.ds(c, 8, stride=8), :] = value
            final = rows[8:48].astype(BF)
            out_ref[t, big_row] = final
            if big_row == 3:
                out_ref[t, 4] = final


def on_device(
    latent,
    proj_weight,
    first_gain,
    first_shift,
    half_weight,
    second_gain,
    second_shift,
    full_weight,
    full_bias,
    anchors,
    reach,
):
    lat = latent.transpose(1, 2, 3, 0, 4).reshape(LCW, 2, 16)
    shard = full_weight.transpose(0, 2, 1)
    any_space = pl.BlockSpec(memory_space=pl.ANY)
    vmem = pl.BlockSpec(memory_space=pltpu.VMEM)
    smem = pl.BlockSpec(memory_space=pltpu.SMEM)
    dma = pltpu.SemaphoreType.DMA
    mid, moments, wc = pl.pallas_call(
        front_kernel,
        name="front",
        out_shape=(
            jax.ShapeDtypeStruct((27, 32, 256), F32),
            jax.ShapeDtypeStruct((8, 256), F32),
            jax.ShapeDtypeStruct((5, 640, 768), BF),
        ),
        in_specs=[any_space] * 8,
        out_specs=(vmem, vmem, vmem),
        scratch_shapes=[
            pltpu.VMEM((3, LCW + 2, 2, 16), BF),
            pltpu.VMEM((16, 256), BF),
            pltpu.VMEM((1, 256), F32),
            pltpu.VMEM((1, 256), F32),
            pltpu.VMEM((27, 256, 256), BF),
            pltpu.VMEM((NT, 27, 16, 256), BF),
            pltpu.SMEM((TILES + 1,), jnp.int32),
            pltpu.SMEM((TILES + 1,), jnp.int32),
            pltpu.VMEM((48, 16), F32),
            pltpu.VMEM((8, 1, 128), F32),
            pltpu.VMEM((24, 1, 128), F32),
            pltpu.VMEM((8, 1, 128), F32),
            pltpu.VMEM((16, 1, 128), F32),
            dma((10,)),
            dma((8,)), dma((8,)), dma((24,)), dma((24,)),
            dma((8,)), dma((8,)), dma((16,)), dma((16,)),
            dma((9,)), dma((9,)), dma((4,)), dma((4,)), dma((4,)), dma((4,)),
        ],
        compiler_params=pltpu.CompilerParams(
            collective_id=0, has_side_effects=True, vmem_limit_bytes=20 * 2**20
        ),
    )(
        lat, proj_weight, first_gain.reshape(1, 256), first_shift.reshape(1, 256),
        half_weight, shard, anchors, reach,
    )
    out = pl.pallas_call(
        back_kernel,
        name="back",
        out_shape=jax.ShapeDtypeStruct((2, 8, 8 * LCW, 128), BF),
        in_specs=[vmem] * 6 + [smem] * 2,
        out_specs=vmem,
        scratch_shapes=[
            pltpu.VMEM((432, 768), BF),
            pltpu.VMEM((49, 48, 128), F32),
            pltpu.VMEM((64, 128), F32),
        ],
        compiler_params=pltpu.CompilerParams(vmem_limit_bytes=20 * 2**20),
    )(
        mid, moments, wc, second_gain.reshape(1, 256), second_shift.reshape(1, 256),
        full_bias.reshape(1, 128), anchors, reach,
    )
    return out[:, None]


def solution(mesh):
    return jax.shard_map(
        on_device,
        mesh=mesh,
        in_specs=(
            P("tm", "tile", None, None, None),
            P(),
            P(),
            P(),
            P(),
            P(),
            P(),
            P(None, None, "tm"),
            P(),
            P(),
            P(),
        ),
        out_specs=P("tm", "tile", None, None, None),
        check_vma=False,
    )
```

```python
import jax
import jax.numpy as jnp
from jax import lax
from jax.experimental import pallas as pl
from jax.experimental.pallas import tpu as pltpu
from jax.sharding import PartitionSpec as P

GROUPS = 32
NX, NZH, NY, NT = 4, 2, 8, 8
TILES = NX * NZH * NY
LCW = 5
BF = jnp.bfloat16
F32 = jnp.float32
MESH = pl.DeviceIdType.MESH

COMBOS = ("01", "12", "0", "2", "012")
ROW_USES = {
    "01": ((0, 1), (1, 5), (2, 7)),
    "12": ((0, 0), (1, 2), (2, 6)),
    "0": ((0, 2), (1, 6)),
    "2": ((1, 1), (2, 5)),
    "012": ((1, 3),),
}
COL_USES = {
    "01": ((0, 1, 0), (1, 5, 0), (2, 7, 0)),
    "12": ((0, 0, 0), (1, 2, 0), (2, 6, 0)),
    "0": ((0, 2, 0), (1, 6, 0), (2, 0, 1)),
    "2": ((0, 7, -1), (1, 1, 0), (2, 5, 0)),
    "012": ((1, 3, 0),),
}
SLOT = {0: 0, 1: 1, 2: 2, 3: 3, 4: 3, 5: 4, 6: 5, 7: 6}


def dot(a, b):
    return jnp.dot(a, b, preferred_element_type=F32)


def exact_dot(x, ones):
    high = x.astype(BF)
    rest = x - high.astype(F32)
    middle = rest.astype(BF)
    low = (rest - middle.astype(F32)).astype(BF)
    return dot(high, ones) + dot(middle, ones) + dot(low, ones)


def iota(shape, dim):
    return lax.broadcasted_iota(jnp.int32, shape, dim)


def encode(sums, squares):
    channel, lane = iota((256, 128), 0), iota((256, 128), 1)
    ones = jnp.where(((channel >> 3) == (lane & 31)) & (lane < 64), 1.0, 0.0).astype(BF)
    row = iota((8, 256), 0)
    stacked = jnp.where(row == 0, sums, jnp.where(row == 1, squares, 0.0))
    coded = exact_dot(stacked, ones)
    return jnp.where(iota((1, 128), 1) < 32, coded[0:1], coded[1:2])


def decode(totals, count):
    lane, channel = iota((128, 256), 0), iota((128, 256), 1)
    ones = jnp.where(((channel >> 3) == (lane & 31)) & (lane < 64), 1.0, 0.0).astype(BF)
    row, place = iota((8, 128), 0), iota((8, 128), 1)
    stacked = jnp.zeros((8, 128), F32)
    for i, total in enumerate(totals):
        stacked = jnp.where((row == 2 * i) & (place < 32), total, stacked)
        stacked = jnp.where((row == 2 * i + 1) & (place >= 32), total, stacked)
    wide = exact_dot(stacked, ones)
    result = []
    for i in range(len(totals)):
        mean = wide[2 * i : 2 * i + 1] / count
        variance = wide[2 * i + 1 : 2 * i + 2] / count - mean * mean
        result.append((mean, lax.rsqrt(variance + 1e-06)))
    return result


def normalize(values, mean, scale, gain, shift):
    v = gain * (values - mean) * scale + shift
    half = 0.5 * v
    return half + half * jnp.tanh(half)


def tile_at(y, z, x):
    return y * (NZH * NX) + z * NX + x


def around(j, k):
    other = j + k
    return jnp.clip(other, 0, TILES - 1), (other >= 0) & (other < TILES)


def blend_weight(columns, low, high, low_reach, high_reach):
    left_edge, right_edge = 8 * low, 8 * high
    left_reach, right_reach = 8 * low_reach, 8 * high_reach
    place = columns.astype(F32)
    rising = jnp.clip(
        (place - (left_edge - left_reach).astype(F32) + 0.5)
        / jnp.maximum(2 * left_reach, 1).astype(F32),
        0.0,
        1.0,
    )
    rising = jnp.where(left_reach > 0, rising, jnp.where(columns >= left_edge, 1.0, 0.0))
    falling = jnp.clip(
        ((right_edge + right_reach).astype(F32) - place - 0.5)
        / jnp.maximum(2 * right_reach, 1).astype(F32),
        0.0,
        1.0,
    )
    falling = jnp.where(right_reach > 0, falling, jnp.where(columns < right_edge, 1.0, 0.0))
    return jnp.minimum(rising, falling)


def front_kernel(
    lat_hbm, wp_hbm, gain_hbm, shift_hbm, hw_hbm, fw_hbm, anchors_hbm, reach_hbm,
    gain2_hbm, shift2_hbm, bias_hbm,
    mid_ref, params_ref, inside_ref, blend_ref, wc_ref,
    lbuf, wp, gain, shift, hw, wt, anchors, reach, gain2, shift2, bias, fl, a1, b1, a2, b2,
    local_sem, sa1, ra1, sb1, rb1, sa2, ra2, sb2, rb2, sl, rl, sw, rw, ss, rs,
):
    j = lax.axis_index("tile")
    tm = lax.axis_index("tm")
    y, z, x = j // (NZH * NX), (j // NX) % NZH, j % NX
    zl = tm // 2

    loads = [
        pltpu.make_async_copy(src, dst, local_sem.at[i])
        for i, (src, dst) in enumerate(
            (
                (lat_hbm, lbuf.at[0, pl.ds(1, LCW)]),
                (wp_hbm, wp),
                (fw_hbm, wt.at[tm]),
                (anchors_hbm, anchors),
                (reach_hbm, reach),
                (gain_hbm, gain),
                (shift_hbm, shift),
                (gain2_hbm, gain2),
                (shift2_hbm, shift2),
                (bias_hbm, bias),
                (hw_hbm.at[pl.ds(0, 9)], hw.at[pl.ds(0, 9)]),
                (hw_hbm.at[pl.ds(9, 9)], hw.at[pl.ds(9, 9)]),
                (hw_hbm.at[pl.ds(18, 9)], hw.at[pl.ds(18, 9)]),
            )
        )
    ]
    for load in loads:
        load.start()

    column = [(tile_at((y + d) % NY, z, x), tm) for d in range(NY)]
    plane = [(s, dz, dx) for s in range(3) for dz in range(NZH) for dx in range(NX)][1:]

    def plane_at(sign, s, dz, dx):
        return (
            tile_at(y, (z + dz) % NZH, (x + sign * dx + NX) % NX),
            (tm + sign * s + NT) % NT,
        )

    def chip_at(step):
        far = (zl + step + 4) // 4
        return (tile_at(y, (z + far + 1) % NZH, x), (tm + 2 * step + NT) % NT)

    sibling = (j, tm + 1 - 2 * (tm % 2))
    chips = [chip_at(1), chip_at(-1), chip_at(2), chip_at(-2)]

    barrier = pltpu.get_barrier_semaphore()
    greeted = column[1:] + [plane_at(-1, *p) for p in plane] + chips + [sibling]
    for s in range(3):
        greeted.append(((j + 1) % TILES, (tm - s + NT) % NT))
        greeted.append(((j + TILES - 1) % TILES, (tm - s + NT) % NT))
    for peer in greeted:
        pl.semaphore_signal(barrier, inc=1, device_id=peer, device_id_type=MESH)

    fl[...] = jnp.zeros_like(fl)
    loads[0].wait()
    loads[1].wait()
    for c in range(LCW):
        fl[pl.ds(32 + 1 + c, 2, stride=8), :] = lbuf[0, 1 + c].astype(F32)
    own = dot(fl[32:48].astype(BF), wp[...])
    a1[0] = encode(jnp.sum(own, axis=0, keepdims=True), jnp.sum(own * own, axis=0, keepdims=True))

    pl.semaphore_wait(barrier, len(greeted))

    def send(src, dst, send_sem, recv_sem, peer):
        copy = pltpu.make_async_remote_copy(
            src_ref=src, dst_ref=dst, send_sem=send_sem, recv_sem=recv_sem,
            device_id=peer, device_id_type=MESH,
        )
        copy.start()
        return copy

    def send_column(buf, s_sem, r_sem):
        return [send(buf.at[0], buf.at[d], s_sem.at[d], r_sem.at[d], column[d]) for d in range(1, NY)]

    def send_plane(buf, s_sem, r_sem, shifts):
        copies = []
        for s, dz, dx in plane:
            if s < shifts:
                i = s * 8 + dz * NX + dx
                copies.append(
                    send(buf.at[0], buf.at[i], s_sem.at[i], r_sem.at[i], plane_at(1, s, dz, dx))
                )
        return copies

    sent = []
    first_column = send_column(a1, sa1, ra1)
    lat_copies = []
    for s in range(3):
        for i, (src, dst, tile) in enumerate(
            (
                (lbuf.at[0, LCW], lbuf.at[s, 0], (j + 1) % TILES),
                (lbuf.at[0, 1], lbuf.at[s, LCW + 1], (j + TILES - 1) % TILES),
                (lbuf.at[0, pl.ds(1, LCW)], lbuf.at[s, pl.ds(1, LCW)], j),
            )
        ):
            if i == 2 and s == 0:
                continue
            n = 3 * s + i
            lat_copies.append(send(src, dst, sl.at[n], rl.at[n], (tile, (tm + s) % NT)))
    loads[2].wait()
    sibling_copies = [send(wt.at[tm], wt.at[tm], ss.at[0], rs.at[0], sibling)]

    for copy in first_column:
        copy.wait_recv()
    b1[0] = jnp.sum(a1[...], axis=0)
    first_plane = send_plane(b1, sb1, rb1, 3)

    half = 14
    chip_copies = [
        send(wt.at[tm], wt.at[tm], sw.at[0], rw.at[0], chips[0]),
        send(wt.at[tm], wt.at[tm], sw.at[1], rw.at[1], chips[1]),
        send(wt.at[tm, pl.ds(0, half)], wt.at[tm, pl.ds(0, half)], sw.at[2], rw.at[2], chips[2]),
        send(
            wt.at[tm, pl.ds(half, 27 - half)], wt.at[tm, pl.ds(half, 27 - half)],
            sw.at[3], rw.at[3], chips[3],
        ),
    ]

    for copy in lat_copies:
        copy.wait_recv()
    for s in range(3):
        for c in range(LCW + 2):
            fl[pl.ds(16 * (2 - s) + c, 2, stride=8), :] = lbuf[s, c].astype(F32)
    projected = dot(fl[...].astype(BF), wp[...])
    for load in loads[3:]:
        load.wait()

    params_ref[4:5] = gain2[...]
    params_ref[5:6] = shift2[...]
    params_ref[6:7, 0:128] = bias[...]
    col = 5 * j - 1 + (iota((32, 256), 0) & 7)
    local_col = iota((32, 256), 0) & 7
    masks, cores = [], []
    for k in (-1, 0, 1):
        t, there = around(j, k)
        low, high = anchors[t], anchors[t + 1]
        inside = (col >= low - reach[t]) & (col < high + reach[t + 1])
        masks.append(jnp.where(inside, 1.0, 0.0))
        inside_ref[k + 1] = masks[-1][0:16]
        there = jnp.where(there, 1, 0)
        core = (col >= low) & (col < high) & (local_col >= 1) & (local_col <= LCW)
        cores.append(jnp.where(core, there.astype(F32), 0.0))

    for c in range(8):
        columns = 40 * j - 8 + 8 * iota((8, 128), 0) + c
        parts = []
        for k in range(3):
            t, there = around(j, k - 1)
            weight = blend_weight(columns, anchors[t], anchors[t + 1], reach[t], reach[t + 1])
            parts.append(weight * jnp.where(there, 1, 0).astype(F32))
        total = parts[0] + parts[1] + parts[2]
        keep = (iota((8, 128), 0) >= 1) & (iota((8, 128), 0) <= LCW)
        total = jnp.where(keep, total, 1.0)
        for k in range(3):
            blend_ref[3 * c + k] = parts[k] / total

    for copy in first_plane:
        copy.wait_recv()
    totals = [jnp.sum(b1[8 * s : 8 * s + 8], axis=0) for s in range(3)]
    stats = decode(totals, float(2 * LCW * TILES * 8))
    frames = []
    for s in (2, 1, 0):
        block = normalize(
            projected[16 * (2 - s) : 16 * (2 - s) + 16], stats[s][0], stats[s][1], gain[...], shift[...]
        )
        frames += [block[0:8], block[8:16]]
    frames[2] = jnp.where(tm == 0, frames[4], frames[2])
    frames[3] = jnp.where(tm == 0, frames[4], frames[3])
    frames[0] = jnp.where(tm == 1, frames[2], frames[0])
    frames[1] = jnp.where(tm == 1, frames[2], frames[1])
    seqs = [jnp.concatenate(frames[a : a + 4], axis=0).astype(BF) for a in range(3)]

    taps = [
        [
            dot(seqs[0], hw[3 * b + d]) + dot(seqs[1], hw[9 + 3 * b + d]) + dot(seqs[2], hw[18 + 3 * b + d])
            for d in range(3)
        ]
        for b in range(3)
    ]
    sums = jnp.zeros((8, 256), F32)
    squares = jnp.zeros((8, 256), F32)

    def rolled(v, by):
        return pltpu.roll(v.reshape(4, 8, 256), by % 8, 1).reshape(32, 256)

    for r in range(3):
        if r == 0:
            q = [taps[1][d] + taps[2][d] for d in range(3)]
        elif r == 1:
            q = [taps[0][d] + taps[1][d] + taps[2][d] for d in range(3)]
        else:
            q = [taps[0][d] + taps[1][d] for d in range(3)]
        right = q[1] + q[2]
        left = q[0] + q[1]
        whole = left + q[2]
        for k in range(3):
            m = masks[k]
            kinds = (
                rolled(m * q[0], 1) + m * right,
                m * whole,
                m * left + rolled(m * q[2], -1),
            )
            for p in range(3):
                mid_ref[k * 9 + r * 3 + p] = kinds[p]
                times = (2.0 if r == 1 else 1.0) * (2.0 if p == 1 else 1.0)
                part = cores[k][16:32] * kinds[p][16:32]
                square = part * kinds[p][16:32]
                sums = sums + times * (part[0:8] + part[8:16])
                squares = squares + times * (square[0:8] + square[8:16])
    a2[0] = encode(jnp.sum(sums, axis=0, keepdims=True), jnp.sum(squares, axis=0, keepdims=True))
    second_column = send_column(a2, sa2, ra2)

    for copy in chip_copies:
        copy.wait_recv()
    for i, shard in enumerate(((tm + 2) % NT, (tm + 4) % NT, (tm + 6) % NT)):
        sibling_copies.append(
            send(wt.at[shard], wt.at[shard], ss.at[1 + i], rs.at[1 + i], sibling)
        )

    for copy in second_column:
        copy.wait_recv()
    b2[0] = jnp.sum(a2[...], axis=0)
    second_plane = send_plane(b2, sb2, rb2, 2)

    for copy in sibling_copies:
        copy.wait_recv()

    def combine(i, carry):
        a, n = i // NT, i % NT
        w = [[wt[n, 9 * a + 3 * b + d].astype(F32) for d in range(3)] for b in range(3)]

        def combos(u):
            first = u[0] + u[1]
            return {"0": u[0], "2": u[2], "01": first, "12": u[1] + u[2], "012": first + u[2]}

        by_col = [combos([w[b][d] for b in range(3)]) for d in range(3)]
        for rc, row_class in enumerate(COMBOS):
            both = combos([by_col[d][row_class] for d in range(3)])
            for cc, col_class in enumerate(COMBOS):
                wc_ref[
                    rc,
                    pl.ds(pl.multiple_of(cc * 128 + n * 16, 16), 16),
                    pl.ds(pl.multiple_of(a * 256, 256), 256),
                ] = both[col_class].astype(BF)
        return carry

    lax.fori_loop(0, 3 * NT, combine, 0)

    for copy in second_plane:
        copy.wait_recv()
    totals = [jnp.sum(b2[8 * s : 8 * s + 8], axis=0) for s in range(2)]
    stats = decode(totals, float(2 * 16 * LCW * TILES * 8))
    params_ref[0:1] = stats[1][0]
    params_ref[1:2] = stats[1][1]
    params_ref[2:3] = stats[0][0]
    params_ref[3:4] = stats[0][1]
    for copy in (
        first_column + lat_copies + first_plane + chip_copies + second_column + sibling_copies + second_plane
    ):
        copy.wait_send()


def back_kernel(
    mid, params, inside, blend, wc, out_ref, xs, acc, rows
):
    tm = lax.axis_index("tm")
    gain, shift, bias = params[4:5], params[5:6], params[6:7, 0:128]
    for k in range(3):
        keep = inside[k]
        for r in range(3):
            for p in range(3):
                values = mid[k * 9 + r * 3 + p]
                before = normalize(values[0:16], params[0:1], params[1:2], gain, shift)
                now = normalize(values[16:32], params[2:3], params[3:4], gain, shift)
                now = keep * now
                before = keep * before
                first = jnp.concatenate([now[0:8], now[0:8]], axis=0)
                before = jnp.where(tm == 0, first, before)
                at = (r * 3 + p) * 48 + k * 16
                xs[at : at + 16, 0:256] = before.astype(BF)
                xs[at : at + 16, 256:512] = jnp.concatenate([before[8:16], now[0:8]], axis=0).astype(BF)
                xs[at : at + 16, 512:768] = now.astype(BF)

    seen = set()
    for rc, row_class in enumerate(COMBOS):
        uses = ROW_USES[row_class]
        r0, r1 = uses[0][0], uses[-1][0] + 1
        for pair in ((0, 1), (2, 3), (4,)):
            if pair == (4,):
                lhs = [xs[r * 144 + 48 : r * 144 + 96] for r in range(r0, r1)]
                lhs = lhs[0] if len(lhs) == 1 else jnp.concatenate(lhs, axis=0)
                inputs = (1,)
            else:
                lhs = xs[r0 * 144 : r1 * 144]
                inputs = (0, 1, 2)
            rhs = wc[rc, pair[0] * 128 : (pair[-1] + 1) * 128]
            result = lax.dot_general(
                lhs, rhs, (((1,), (1,)), ((), ())), preferred_element_type=F32
            )
            for r, big_row in uses:
                for half, cc in enumerate(pair):
                    for p, big_col, by in COL_USES[COMBOS[cc]]:
                        at = ((r - r0) * len(inputs) + inputs.index(p)) * 48
                        part = result[at : at + 48, half * 128 : half * 128 + 128]
                        if by:
                            part = pltpu.roll(part.reshape(6, 8, 128), by % 8, 1).reshape(48, 128)
                        slot = SLOT[big_row] * 7 + SLOT[big_col]
                        if slot in seen:
                            acc[slot] += part
                        else:
                            seen.add(slot)
                            acc[slot] = part

    for t in range(2):
        for big_row in (0, 1, 2, 3, 5, 6, 7):
            for c in range(8):
                slot = SLOT[big_row] * 7 + SLOT[c]
                value = None
                for k in range(3):
                    at = k * 16 + t * 8
                    piece = (acc[slot, at : at + 8] + bias).astype(BF).astype(F32) * blend[3 * c + k]
                    value = piece if value is None else value + piece
                rows[pl.ds(c, 8, stride=8), :] = value
            final = rows[8:48].astype(BF)
            out_ref[t, big_row] = final
            if big_row == 3:
                out_ref[t, 4] = final


def on_device(
    latent,
    proj_weight,
    first_gain,
    first_shift,
    half_weight,
    second_gain,
    second_shift,
    full_weight,
    full_bias,
    anchors,
    reach,
):
    lat = latent.transpose(1, 2, 3, 0, 4).reshape(LCW, 2, 16)
    shard = full_weight.transpose(0, 2, 1)
    any_space = pl.BlockSpec(memory_space=pl.ANY)
    vmem = pl.BlockSpec(memory_space=pltpu.VMEM)
    dma = pltpu.SemaphoreType.DMA
    held = pl.pallas_call(
        front_kernel,
        name="front",
        out_shape=(
            jax.ShapeDtypeStruct((27, 32, 256), F32),
            jax.ShapeDtypeStruct((8, 256), F32),
            jax.ShapeDtypeStruct((3, 16, 256), F32),
            jax.ShapeDtypeStruct((24, 8, 128), F32),
            jax.ShapeDtypeStruct((5, 640, 768), BF),
        ),
        in_specs=[any_space] * 11,
        out_specs=(vmem,) * 5,
        scratch_shapes=[
            pltpu.VMEM((3, LCW + 2, 2, 16), BF),
            pltpu.VMEM((16, 256), BF),
            pltpu.VMEM((1, 256), F32),
            pltpu.VMEM((1, 256), F32),
            pltpu.VMEM((27, 256, 256), BF),
            pltpu.VMEM((NT, 27, 16, 256), BF),
            pltpu.SMEM((TILES + 1,), jnp.int32),
            pltpu.SMEM((TILES + 1,), jnp.int32),
            pltpu.VMEM((1, 256), F32),
            pltpu.VMEM((1, 256), F32),
            pltpu.VMEM((1, 128), F32),
            pltpu.VMEM((48, 16), F32),
            pltpu.VMEM((8, 1, 128), F32),
            pltpu.VMEM((24, 1, 128), F32),
            pltpu.VMEM((8, 1, 128), F32),
            pltpu.VMEM((16, 1, 128), F32),
            dma((13,)),
            dma((8,)), dma((8,)), dma((24,)), dma((24,)),
            dma((8,)), dma((8,)), dma((16,)), dma((16,)),
            dma((9,)), dma((9,)), dma((4,)), dma((4,)), dma((4,)), dma((4,)),
        ],
        compiler_params=pltpu.CompilerParams(
            collective_id=0, has_side_effects=True, vmem_limit_bytes=20 * 2**20
        ),
    )(
        *(
            pltpu.with_memory_space_constraint(v, pltpu.HBM)
            for v in (
                lat, proj_weight, first_gain.reshape(1, 256), first_shift.reshape(1, 256),
                half_weight, shard, anchors, reach,
                second_gain.reshape(1, 256), second_shift.reshape(1, 256), full_bias.reshape(1, 128),
            )
        )
    )
    out = pl.pallas_call(
        back_kernel,
        name="back",
        out_shape=jax.ShapeDtypeStruct((2, 8, 8 * LCW, 128), BF),
        in_specs=[vmem] * 5,
        out_specs=vmem,
        scratch_shapes=[
            pltpu.VMEM((432, 768), BF),
            pltpu.VMEM((49, 48, 128), F32),
            pltpu.VMEM((64, 128), F32),
        ],
        compiler_params=pltpu.CompilerParams(vmem_limit_bytes=20 * 2**20),
    )(*held)
    return out[:, None]


def solution(mesh):
    return jax.shard_map(
        on_device,
        mesh=mesh,
        in_specs=(
            P("tm", "tile", None, None, None),
            P(),
            P(),
            P(),
            P(),
            P(),
            P(),
            P(None, None, "tm"),
            P(),
            P(),
            P(),
        ),
        out_specs=P("tm", "tile", None, None, None),
        check_vma=False,
    )
```

```python
import jax
import jax.numpy as jnp
from jax import lax
from jax.experimental import pallas as pl
from jax.experimental.pallas import tpu as pltpu
from jax.sharding import PartitionSpec as P

GROUPS = 32
NX, NZH, NY, NT = 4, 2, 8, 8
TILES = NX * NZH * NY
LCW = 5
BF = jnp.bfloat16
F32 = jnp.float32
MESH = pl.DeviceIdType.MESH


def dot(a, b):
    return jnp.dot(a, b, preferred_element_type=F32)


def exact_dot(x, ones):
    high = x.astype(BF)
    rest = x - high.astype(F32)
    middle = rest.astype(BF)
    low = (rest - middle.astype(F32)).astype(BF)
    return dot(high, ones) + dot(middle, ones) + dot(low, ones)


def iota(shape, dim):
    return lax.broadcasted_iota(jnp.int32, shape, dim)


def encode(sums, squares):
    channel, lane = iota((256, 128), 0), iota((256, 128), 1)
    ones = jnp.where(((channel >> 3) == (lane & 31)) & (lane < 64), 1.0, 0.0).astype(BF)
    row = iota((8, 256), 0)
    stacked = jnp.where(row == 0, sums, jnp.where(row == 1, squares, 0.0))
    coded = exact_dot(stacked, ones)
    return jnp.where(iota((1, 128), 1) < 32, coded[0:1], coded[1:2])


def decode(totals, count):
    lane, channel = iota((128, 256), 0), iota((128, 256), 1)
    ones = jnp.where(((channel >> 3) == (lane & 31)) & (lane < 64), 1.0, 0.0).astype(BF)
    row, place = iota((8, 128), 0), iota((8, 128), 1)
    stacked = jnp.zeros((8, 128), F32)
    for i, total in enumerate(totals):
        stacked = jnp.where((row == 2 * i) & (place < 32), total, stacked)
        stacked = jnp.where((row == 2 * i + 1) & (place >= 32), total, stacked)
    wide = exact_dot(stacked, ones)
    result = []
    for i in range(len(totals)):
        mean = wide[2 * i : 2 * i + 1] / count
        variance = wide[2 * i + 1 : 2 * i + 2] / count - mean * mean
        result.append((mean, lax.rsqrt(variance + 1e-06)))
    return result


def normalize(values, mean, scale, gain, shift):
    v = gain * (values - mean) * scale + shift
    half = 0.5 * v
    return half + half * jnp.tanh(half)


def tile_at(y, z, x):
    return y * (NZH * NX) + z * NX + x


def around(j, k):
    other = j + k
    return jnp.clip(other, 0, TILES - 1), (other >= 0) & (other < TILES)


def blend_weight(columns, low, high, low_reach, high_reach):
    left_edge, right_edge = 8 * low, 8 * high
    left_reach, right_reach = 8 * low_reach, 8 * high_reach
    place = columns.astype(F32)
    rising = jnp.clip(
        (place - (left_edge - left_reach).astype(F32) + 0.5)
        / jnp.maximum(2 * left_reach, 1).astype(F32),
        0.0,
        1.0,
    )
    rising = jnp.where(left_reach > 0, rising, jnp.where(columns >= left_edge, 1.0, 0.0))
    falling = jnp.clip(
        ((right_edge + right_reach).astype(F32) - place - 0.5)
        / jnp.maximum(2 * right_reach, 1).astype(F32),
        0.0,
        1.0,
    )
    falling = jnp.where(right_reach > 0, falling, jnp.where(columns < right_edge, 1.0, 0.0))
    return jnp.minimum(rising, falling)


def front_kernel(
    lat_hbm, wp_hbm, gain_hbm, shift_hbm, hw_hbm, fw_hbm, anchors_hbm, reach_hbm,
    gain2_hbm, shift2_hbm, bias_hbm,
    mid_ref, params_ref, inside_ref, blend_ref, wc_ref,
    lbuf, wp, gain, shift, hw, wt, anchors, reach, gain2, shift2, bias, fl, a1, b1, a2, b2,
    local_sem, sa1, ra1, sb1, rb1, sa2, ra2, sb2, rb2, sl, rl, sw, rw, ss, rs,
):
    j = lax.axis_index("tile")
    tm = lax.axis_index("tm")
    y, z, x = j // (NZH * NX), (j // NX) % NZH, j % NX
    zl = tm // 2

    loads = [
        pltpu.make_async_copy(src, dst, local_sem.at[i])
        for i, (src, dst) in enumerate(
            (
                (lat_hbm, lbuf.at[pl.ds(1, LCW)]),
                (wp_hbm, wp),
                (fw_hbm, wt.at[tm]),
                (anchors_hbm, anchors),
                (reach_hbm, reach),
                (gain_hbm, gain),
                (shift_hbm, shift),
                (gain2_hbm, gain2),
                (shift2_hbm, shift2),
                (bias_hbm, bias),
                (hw_hbm.at[pl.ds(0, 9)], hw.at[pl.ds(0, 9)]),
                (hw_hbm.at[pl.ds(9, 9)], hw.at[pl.ds(9, 9)]),
                (hw_hbm.at[pl.ds(18, 9)], hw.at[pl.ds(18, 9)]),
            )
        )
    ]
    for load in loads:
        load.start()

    column = [(tile_at((y + d) % NY, z, x), tm) for d in range(NY)]
    plane = [(s, dz, dx) for s in range(3) for dz in range(NZH) for dx in range(NX)][1:]

    def plane_at(sign, s, dz, dx):
        return (
            tile_at(y, (z + dz) % NZH, (x + sign * dx + NX) % NX),
            (tm + sign * s + NT) % NT,
        )

    def chip_at(step):
        far = (zl + step + 4) // 4
        return (tile_at(y, (z + far + 1) % NZH, x), (tm + 2 * step + NT) % NT)

    sibling = (j, tm + 1 - 2 * (tm % 2))
    chips = [chip_at(1), chip_at(-1), chip_at(2), chip_at(-2)]

    barrier = pltpu.get_barrier_semaphore()
    greeted = column[1:] + [plane_at(-1, *p) for p in plane] + chips + [sibling]
    for s in range(3):
        greeted.append(((j + 1) % TILES, (tm - s + NT) % NT))
        greeted.append(((j + TILES - 1) % TILES, (tm - s + NT) % NT))
    for peer in greeted:
        pl.semaphore_signal(barrier, inc=1, device_id=peer, device_id_type=MESH)

    fl[...] = jnp.zeros_like(fl)
    loads[0].wait()
    loads[1].wait()
    for c in range(LCW):
        fl[pl.ds(32 + 1 + c, 2, stride=8), :] = lbuf[1 + c].astype(F32)
    own = dot(fl[32:48].astype(BF), wp[...])
    a1[0] = encode(jnp.sum(own, axis=0, keepdims=True), jnp.sum(own * own, axis=0, keepdims=True))

    pl.semaphore_wait(barrier, len(greeted))

    def send(src, dst, send_sem, recv_sem, peer):
        pltpu.make_async_remote_copy(
            src_ref=src, dst_ref=dst, send_sem=send_sem, recv_sem=recv_sem,
            device_id=peer, device_id_type=MESH,
        ).start()

    def await_all(part, sem):
        pltpu.make_async_copy(part, part, sem).wait()

    def send_column(buf, s_sem, r_sem):
        for d in range(1, NY):
            send(buf.at[0], buf.at[d], s_sem, r_sem, column[d])

    def send_plane(buf, s_sem, r_sem, shifts):
        for s, dz, dx in plane:
            if s < shifts:
                send(buf.at[0], buf.at[s * 8 + dz * NX + dx], s_sem, r_sem, plane_at(1, s, dz, dx))

    send_column(a1, sa1, ra1)
    for s in range(3):
        first = s * (LCW + 2)
        for i, (src, dst, tile) in enumerate(
            (
                (lbuf.at[LCW], lbuf.at[first], (j + 1) % TILES),
                (lbuf.at[1], lbuf.at[first + LCW + 1], (j + TILES - 1) % TILES),
                (lbuf.at[pl.ds(1, LCW)], lbuf.at[pl.ds(first + 1, LCW)], j),
            )
        ):
            if i == 2 and s == 0:
                continue
            send(src, dst, sl, rl, (tile, (tm + s) % NT))
    loads[2].wait()
    send(wt.at[tm], wt.at[tm], ss, rs, sibling)

    await_all(a1.at[pl.ds(1, 7)], ra1)
    b1[0] = jnp.sum(a1[...], axis=0)
    send_plane(b1, sb1, rb1, 3)

    half = 14
    send(wt.at[tm], wt.at[tm], sw, rw, chips[0])
    send(wt.at[tm], wt.at[tm], sw, rw, chips[1])
    for first, many, chip in ((0, half, chips[2]), (half, 27 - half, chips[3])):
        part = wt.at[tm, pl.ds(first, many)]
        send(part, part, sw, rw, chip)

    await_all(lbuf.at[pl.ds(0, 16)], rl)
    for s in range(3):
        for c in range(LCW + 2):
            fl[pl.ds(16 * (2 - s) + c, 2, stride=8), :] = lbuf[s * (LCW + 2) + c].astype(F32)
    projected = dot(fl[...].astype(BF), wp[...])
    for load in loads[3:]:
        load.wait()

    params_ref[4:5] = gain2[...]
    params_ref[5:6] = shift2[...]
    params_ref[6:7, 0:128] = bias[...]
    col = 5 * j - 1 + (iota((32, 256), 0) & 7)
    local_col = iota((32, 256), 0) & 7
    masks, cores = [], []
    for k in (-1, 0, 1):
        t, there = around(j, k)
        low, high = anchors[t], anchors[t + 1]
        inside = (col >= low - reach[t]) & (col < high + reach[t + 1])
        masks.append(jnp.where(inside, 1.0, 0.0))
        inside_ref[k + 1] = masks[-1][0:16]
        there = jnp.where(there, 1, 0)
        core = (col >= low) & (col < high) & (local_col >= 1) & (local_col <= LCW)
        cores.append(jnp.where(core, there.astype(F32), 0.0))

    for c in range(8):
        columns = 40 * j - 8 + 8 * iota((8, 128), 0) + c
        parts = []
        for k in range(3):
            t, there = around(j, k - 1)
            weight = blend_weight(columns, anchors[t], anchors[t + 1], reach[t], reach[t + 1])
            parts.append(weight * jnp.where(there, 1, 0).astype(F32))
        total = parts[0] + parts[1] + parts[2]
        keep = (iota((8, 128), 0) >= 1) & (iota((8, 128), 0) <= LCW)
        total = jnp.where(keep, total, 1.0)
        for k in range(3):
            blend_ref[3 * c + k] = parts[k] / total

    await_all(b1.at[pl.ds(1, 23)], rb1)
    totals = [jnp.sum(b1[8 * s : 8 * s + 8], axis=0) for s in range(3)]
    stats = decode(totals, float(2 * LCW * TILES * 8))
    frames = []
    for s in (2, 1, 0):
        block = normalize(
            projected[16 * (2 - s) : 16 * (2 - s) + 16], stats[s][0], stats[s][1], gain[...], shift[...]
        )
        frames += [block[0:8], block[8:16]]
    frames[2] = jnp.where(tm == 0, frames[4], frames[2])
    frames[3] = jnp.where(tm == 0, frames[4], frames[3])
    frames[0] = jnp.where(tm == 1, frames[2], frames[0])
    frames[1] = jnp.where(tm == 1, frames[2], frames[1])
    seqs = [jnp.concatenate(frames[a : a + 4], axis=0).astype(BF) for a in range(3)]

    taps = [
        [
            dot(seqs[0], hw[3 * b + d]) + dot(seqs[1], hw[9 + 3 * b + d]) + dot(seqs[2], hw[18 + 3 * b + d])
            for d in range(3)
        ]
        for b in range(3)
    ]
    sums = jnp.zeros((8, 256), F32)
    squares = jnp.zeros((8, 256), F32)

    def rolled(v, by):
        return pltpu.roll(v.reshape(4, 8, 256), by % 8, 1).reshape(32, 256)

    for r in range(3):
        if r == 0:
            q = [taps[1][d] + taps[2][d] for d in range(3)]
        elif r == 1:
            q = [taps[0][d] + taps[1][d] + taps[2][d] for d in range(3)]
        else:
            q = [taps[0][d] + taps[1][d] for d in range(3)]
        right = q[1] + q[2]
        left = q[0] + q[1]
        whole = left + q[2]
        for k in range(3):
            m = masks[k]
            kinds = (
                rolled(m * q[0], 1) + m * right,
                m * whole,
                m * left + rolled(m * q[2], -1),
            )
            for p in range(3):
                mid_ref[k * 9 + r * 3 + p] = kinds[p]
                times = (2.0 if r == 1 else 1.0) * (2.0 if p == 1 else 1.0)
                part = cores[k][16:32] * kinds[p][16:32]
                square = part * kinds[p][16:32]
                sums = sums + times * (part[0:8] + part[8:16])
                squares = squares + times * (square[0:8] + square[8:16])
    a2[0] = encode(jnp.sum(sums, axis=0, keepdims=True), jnp.sum(squares, axis=0, keepdims=True))
    send_column(a2, sa2, ra2)

    await_all(wt.at[pl.ds(0, 3)], rw)
    for shard in ((tm + 2) % NT, (tm + 4) % NT, (tm + 6) % NT):
        send(wt.at[shard], wt.at[shard], ss, rs, sibling)

    await_all(a2.at[pl.ds(1, 7)], ra2)
    b2[0] = jnp.sum(a2[...], axis=0)
    send_plane(b2, sb2, rb2, 2)

    await_all(wt.at[pl.ds(0, 4)], rs)

    def arrange(n, carry):
        for tap in range(9):
            for a in range(3):
                wc_ref[
                    pl.ds(pl.multiple_of(tap * 128 + n * 16, 16), 16), a * 256 : a * 256 + 256
                ] = wt[n, 9 * a + tap]
        return carry

    lax.fori_loop(0, NT, arrange, 0)

    await_all(b2.at[pl.ds(1, 15)], rb2)
    totals = [jnp.sum(b2[8 * s : 8 * s + 8], axis=0) for s in range(2)]
    stats = decode(totals, float(2 * 16 * LCW * TILES * 8))
    params_ref[0:1] = stats[1][0]
    params_ref[1:2] = stats[1][1]
    params_ref[2:3] = stats[0][0]
    params_ref[3:4] = stats[0][1]
    for part, sem in (
        (a1.at[pl.ds(1, 7)], sa1),
        (b1.at[pl.ds(1, 23)], sb1),
        (lbuf.at[pl.ds(0, 16)], sl),
        (wt.at[pl.ds(0, 3)], sw),
        (wt.at[pl.ds(0, 4)], ss),
        (a2.at[pl.ds(1, 7)], sa2),
        (b2.at[pl.ds(1, 15)], sb2),
    ):
        await_all(part, sem)


def back_kernel(
    mid, params, inside, blend, wc, out_ref, xs, prod, rows
):
    tm = lax.axis_index("tm")
    gain, shift, bias = params[4:5], params[5:6], params[6:7, 0:128]
    for k in range(3):
        keep = inside[k]
        for r in range(3):
            for p in range(3):
                values = mid[k * 9 + r * 3 + p]
                before = normalize(values[0:16], params[0:1], params[1:2], gain, shift)
                now = normalize(values[16:32], params[2:3], params[3:4], gain, shift)
                now = keep * now
                before = keep * before
                first = jnp.concatenate([now[0:8], now[0:8]], axis=0)
                before = jnp.where(tm == 0, first, before)
                at = (r * 3 + p) * 48 + k * 16
                xs[at : at + 16, 0:256] = before.astype(BF)
                xs[at : at + 16, 256:512] = jnp.concatenate([before[8:16], now[0:8]], axis=0).astype(BF)
                xs[at : at + 16, 512:768] = now.astype(BF)

    for n in range(0, 9, 2):
        many = min(2, 9 - n)
        result = lax.dot_general(
            xs[...], wc[n * 128 : (n + many) * 128], (((1,), (1,)), ((), ())), preferred_element_type=F32
        )
        for i in range(many):
            prod[n + i] = result[:, i * 128 : i * 128 + 128]

    def products(b, r, at):
        return [
            [prod[3 * b + d, (r * 3 + p) * 48 + at : (r * 3 + p) * 48 + at + 8] for p in range(3)]
            for d in range(3)
        ]

    for t in range(2):
        for k in range(3):
            at = k * 16 + t * 8
            across = {}
            for b in range(3):
                for r in range(3):
                    (a0, a1, a3), (b0, b1, b3), (c0, c1, c3) = products(b, r, at)
                    ab1, bc1 = a1 + b1, b1 + c1
                    across[b, r] = (
                        pltpu.roll(a3, 1, 0) + (b0 + c0),
                        (a0 + b0) + c1,
                        a0 + bc1,
                        ab1 + c1,
                        ab1 + c3,
                        a1 + (b3 + c3),
                        (a3 + b3) + pltpu.roll(c0, 7, 0),
                    )
            for c in range(7):
                (x0, x1, x3), (y0, y1, y3), (z0, z1, z3) = [
                    [across[b, r][c] for r in range(3)] for b in range(3)
                ]
                xy1, yz1 = x1 + y1, y1 + z1
                down = (
                    y0 + z0,
                    (x0 + y0) + z1,
                    x0 + yz1,
                    xy1 + z1,
                    xy1 + z3,
                    x1 + (y3 + z3),
                    x3 + y3,
                )
                for r in range(7):
                    value = (down[r] + bias).astype(BF).astype(F32)
                    for column in (3, 4) if c == 3 else (c if c < 3 else c + 1,):
                        place = pl.ds(column, 8, stride=8)
                        piece = value * blend[3 * column + k]
                        if k == 0:
                            rows[r, place, :] = piece
                        else:
                            rows[r, place, :] += piece
        for r in range(7):
            final = rows[r, 8:48].astype(BF)
            for big_row in (3, 4) if r == 3 else (r if r < 3 else r + 1,):
                out_ref[t, big_row] = final


def on_device(
    latent,
    proj_weight,
    first_gain,
    first_shift,
    half_weight,
    second_gain,
    second_shift,
    full_weight,
    full_bias,
    anchors,
    reach,
):
    lat = latent.transpose(1, 2, 3, 0, 4).reshape(LCW, 2, 16)
    shard = full_weight.transpose(0, 2, 1)
    any_space = pl.BlockSpec(memory_space=pl.ANY)
    vmem = pl.BlockSpec(memory_space=pltpu.VMEM)
    dma = pltpu.SemaphoreType.DMA
    held = pl.pallas_call(
        front_kernel,
        name="front",
        out_shape=(
            jax.ShapeDtypeStruct((27, 32, 256), F32),
            jax.ShapeDtypeStruct((8, 256), F32),
            jax.ShapeDtypeStruct((3, 16, 256), F32),
            jax.ShapeDtypeStruct((24, 8, 128), F32),
            jax.ShapeDtypeStruct((9 * 128, 768), BF),
        ),
        in_specs=[any_space] * 11,
        out_specs=(vmem,) * 5,
        scratch_shapes=[
            pltpu.VMEM((3 * (LCW + 2), 2, 16), BF),
            pltpu.VMEM((16, 256), BF),
            pltpu.VMEM((1, 256), F32),
            pltpu.VMEM((1, 256), F32),
            pltpu.VMEM((27, 256, 256), BF),
            pltpu.VMEM((NT, 27, 16, 256), BF),
            pltpu.SMEM((TILES + 1,), jnp.int32),
            pltpu.SMEM((TILES + 1,), jnp.int32),
            pltpu.VMEM((1, 256), F32),
            pltpu.VMEM((1, 256), F32),
            pltpu.VMEM((1, 128), F32),
            pltpu.VMEM((48, 16), F32),
            pltpu.VMEM((8, 1, 128), F32),
            pltpu.VMEM((24, 1, 128), F32),
            pltpu.VMEM((8, 1, 128), F32),
            pltpu.VMEM((16, 1, 128), F32),
            dma((13,)),
            *[dma] * 14,
        ],
        compiler_params=pltpu.CompilerParams(
            collective_id=0, has_side_effects=True, vmem_limit_bytes=20 * 2**20
        ),
    )(
        *(
            pltpu.with_memory_space_constraint(v, pltpu.HBM)
            for v in (
                lat, proj_weight, first_gain.reshape(1, 256), first_shift.reshape(1, 256),
                half_weight, shard, anchors, reach,
                second_gain.reshape(1, 256), second_shift.reshape(1, 256), full_bias.reshape(1, 128),
            )
        )
    )
    out = pl.pallas_call(
        back_kernel,
        name="back",
        out_shape=jax.ShapeDtypeStruct((2, 8, 8 * LCW, 128), BF),
        in_specs=[vmem] * 5,
        out_specs=vmem,
        scratch_shapes=[
            pltpu.VMEM((432, 768), BF),
            pltpu.VMEM((9, 432, 128), F32),
            pltpu.VMEM((7, 64, 128), F32),
        ],
        compiler_params=pltpu.CompilerParams(vmem_limit_bytes=20 * 2**20),
    )(*held)
    return out[:, None]


def solution(mesh):
    return jax.shard_map(
        on_device,
        mesh=mesh,
        in_specs=(
            P("tm", "tile", None, None, None),
            P(),
            P(),
            P(),
            P(),
            P(),
            P(),
            P(None, None, "tm"),
            P(),
            P(),
            P(),
        ),
        out_specs=P("tm", "tile", None, None, None),
        check_vma=False,
    )
```

```python
import jax
import jax.numpy as jnp
from jax import lax
from jax.experimental import pallas as pl
from jax.experimental.pallas import tpu as pltpu
from jax.sharding import PartitionSpec as P

GROUPS = 32
NX, NZH, NY, NT = 4, 2, 8, 8
TILES = NX * NZH * NY
LCW = 5
BF = jnp.bfloat16
F32 = jnp.float32
MESH = pl.DeviceIdType.MESH


def dot(a, b):
    return jnp.dot(a, b, preferred_element_type=F32)


def exact_dot(x, ones):
    high = x.astype(BF)
    rest = x - high.astype(F32)
    middle = rest.astype(BF)
    low = (rest - middle.astype(F32)).astype(BF)
    return dot(high, ones) + dot(middle, ones) + dot(low, ones)


def iota(shape, dim):
    return lax.broadcasted_iota(jnp.int32, shape, dim)


def encode(sums, squares):
    channel, lane = iota((256, 128), 0), iota((256, 128), 1)
    ones = jnp.where(((channel >> 3) == (lane & 31)) & (lane < 64), 1.0, 0.0).astype(BF)
    row = iota((8, 256), 0)
    stacked = jnp.where(row == 0, sums, jnp.where(row == 1, squares, 0.0))
    coded = exact_dot(stacked, ones)
    return jnp.where(iota((1, 128), 1) < 32, coded[0:1], coded[1:2])


def decode(totals, count):
    lane, channel = iota((128, 256), 0), iota((128, 256), 1)
    ones = jnp.where(((channel >> 3) == (lane & 31)) & (lane < 64), 1.0, 0.0).astype(BF)
    row, place = iota((8, 128), 0), iota((8, 128), 1)
    stacked = jnp.zeros((8, 128), F32)
    for i, total in enumerate(totals):
        stacked = jnp.where((row == 2 * i) & (place < 32), total, stacked)
        stacked = jnp.where((row == 2 * i + 1) & (place >= 32), total, stacked)
    wide = exact_dot(stacked, ones)
    result = []
    for i in range(len(totals)):
        mean = wide[2 * i : 2 * i + 1] / count
        variance = wide[2 * i + 1 : 2 * i + 2] / count - mean * mean
        result.append((mean, lax.rsqrt(variance + 1e-06)))
    return result


def normalize(values, mean, scale, gain, shift):
    v = gain * (values - mean) * scale + shift
    half = 0.5 * v
    return half + half * jnp.tanh(half)


def tile_at(y, z, x):
    return y * (NZH * NX) + z * NX + x


def around(j, k):
    other = j + k
    return jnp.clip(other, 0, TILES - 1), (other >= 0) & (other < TILES)


def blend_weight(columns, low, high, low_reach, high_reach):
    left_edge, right_edge = 8 * low, 8 * high
    left_reach, right_reach = 8 * low_reach, 8 * high_reach
    place = columns.astype(F32)
    rising = jnp.clip(
        (place - (left_edge - left_reach).astype(F32) + 0.5)
        / jnp.maximum(2 * left_reach, 1).astype(F32),
        0.0,
        1.0,
    )
    rising = jnp.where(left_reach > 0, rising, jnp.where(columns >= left_edge, 1.0, 0.0))
    falling = jnp.clip(
        ((right_edge + right_reach).astype(F32) - place - 0.5)
        / jnp.maximum(2 * right_reach, 1).astype(F32),
        0.0,
        1.0,
    )
    falling = jnp.where(right_reach > 0, falling, jnp.where(columns < right_edge, 1.0, 0.0))
    return jnp.minimum(rising, falling)


def front_kernel(
    lat_hbm, wp_hbm, gain_hbm, shift_hbm, hw_hbm, fw_hbm, anchors_hbm, reach_hbm,
    gain2_hbm, shift2_hbm, bias_hbm,
    mid_ref, params_ref, inside_ref, blend_ref, wc_ref,
    lbuf, wp, gain, shift, hw, wt, anchors, reach, gain2, shift2, bias, fl, a1, b1, b2,
    local_sem, sa1, ra1, sb1, rb1, sb2, rb2, sl, rl, sw, rw, ss, rs,
):
    j = lax.axis_index("tile")
    tm = lax.axis_index("tm")
    y, z, x = j // (NZH * NX), (j // NX) % NZH, j % NX
    zl = tm // 2

    loads = [
        pltpu.make_async_copy(src, dst, local_sem.at[i])
        for i, (src, dst) in enumerate(
            (
                (lat_hbm, lbuf.at[pl.ds(1, LCW)]),
                (wp_hbm, wp),
                (fw_hbm, wt.at[tm]),
                (anchors_hbm, anchors),
                (reach_hbm, reach),
                (gain_hbm, gain),
                (shift_hbm, shift),
                (gain2_hbm, gain2),
                (shift2_hbm, shift2),
                (bias_hbm, bias),
                (hw_hbm.at[pl.ds(0, 9)], hw.at[pl.ds(0, 9)]),
                (hw_hbm.at[pl.ds(9, 9)], hw.at[pl.ds(9, 9)]),
                (hw_hbm.at[pl.ds(18, 9)], hw.at[pl.ds(18, 9)]),
            )
        )
    ]
    for load in loads:
        load.start()

    column = [(tile_at((y + d) % NY, z, x), tm) for d in range(NY)]
    shifts = (0, 1, 2, -1)
    plane = [(i, dz, dx) for i in range(4) for dz in range(NZH) for dx in range(NX)][1:]
    plane.sort(key=lambda p: -(4 * p[1] + min(p[2], NX - p[2])))
    everyone = [
        (s, dy, dz, dx) for s in range(2) for dy in range(NY) for dz in range(NZH) for dx in range(NX)
    ][1:]
    everyone.sort(key=lambda p: -(min(p[1], NY - p[1]) + 4 * p[2] + min(p[3], NX - p[3])))

    def plane_at(sign, i, dz, dx):
        return (
            tile_at(y, (z + dz) % NZH, (x + sign * dx + NX) % NX),
            (tm + sign * shifts[i] + NT) % NT,
        )

    def chip_at(step):
        far = (zl + step + 4) // 4
        return (tile_at(y, (z + far + 1) % NZH, x), (tm + 2 * step + NT) % NT)

    sibling = (j, tm + 1 - 2 * (tm % 2))
    chips = [chip_at(1), chip_at(-1), chip_at(2), chip_at(-2)]

    barrier = pltpu.get_barrier_semaphore()
    greeted = []
    for s in range(3):
        greeted.append(((j + 1) % TILES, (tm - s + NT) % NT))
        greeted.append(((j + TILES - 1) % TILES, (tm - s + NT) % NT))
    greeted += [plane_at(-1, *p) for p in plane] + column[1:] + chips + [sibling]
    for peer in greeted:
        pl.semaphore_signal(barrier, inc=1, device_id=peer, device_id_type=MESH)

    fl[...] = jnp.zeros_like(fl)
    loads[0].wait()
    loads[1].wait()
    for c in range(LCW):
        fl[pl.ds(32 + 1 + c, 2, stride=8), :] = lbuf[1 + c].astype(F32)
    own = dot(fl[32:48].astype(BF), wp[...])
    a1[0] = encode(jnp.sum(own, axis=0, keepdims=True), jnp.sum(own * own, axis=0, keepdims=True))

    pl.semaphore_wait(barrier, len(greeted))

    def send(src, dst, send_sem, recv_sem, peer):
        pltpu.make_async_remote_copy(
            src_ref=src, dst_ref=dst, send_sem=send_sem, recv_sem=recv_sem,
            device_id=peer, device_id_type=MESH,
        ).start()

    def await_all(part, sem):
        pltpu.make_async_copy(part, part, sem).wait()

    def send_column(buf, s_sem, r_sem):
        for d in (4, 3, 5, 2, 6, 1, 7):
            send(buf.at[0], buf.at[d], s_sem, r_sem, column[d])

    send_column(a1, sa1, ra1)
    for s in range(3):
        first = s * (LCW + 2)
        for i, (src, dst, tile) in enumerate(
            (
                (lbuf.at[LCW], lbuf.at[first], (j + 1) % TILES),
                (lbuf.at[1], lbuf.at[first + LCW + 1], (j + TILES - 1) % TILES),
                (lbuf.at[pl.ds(1, LCW)], lbuf.at[pl.ds(first + 1, LCW)], j),
            )
        ):
            if i == 2 and s == 0:
                continue
            send(src, dst, sl, rl, (tile, (tm + s) % NT))
    loads[2].wait()
    send(wt.at[tm], wt.at[tm], ss, rs, sibling)

    await_all(a1.at[pl.ds(1, 7)], ra1)
    b1[0] = jnp.sum(a1[...], axis=0)
    for i, dz, dx in plane:
        send(b1.at[0], b1.at[8 * i + dz * NX + dx], sb1, rb1, plane_at(1, i, dz, dx))

    half = 14
    send(wt.at[tm], wt.at[tm], sw, rw, chips[0])
    send(wt.at[tm], wt.at[tm], sw, rw, chips[1])
    for first, many, chip in ((0, half, chips[2]), (half, 27 - half, chips[3])):
        part = wt.at[tm, pl.ds(first, many)]
        send(part, part, sw, rw, chip)

    await_all(lbuf.at[pl.ds(0, 16)], rl)
    for s in range(3):
        for c in range(LCW + 2):
            fl[pl.ds(16 * (2 - s) + c, 2, stride=8), :] = lbuf[s * (LCW + 2) + c].astype(F32)
    projected = dot(fl[...].astype(BF), wp[...])
    for load in loads[3:]:
        load.wait()

    params_ref[4:5] = gain2[...]
    params_ref[5:6] = shift2[...]
    params_ref[6:7, 0:128] = bias[...]
    col = 5 * j - 1 + (iota((16, 256), 0) & 7)
    local_col = iota((16, 256), 0) & 7
    masks, cores = [], []
    for k in (-1, 0, 1):
        t, there = around(j, k)
        low, high = anchors[t], anchors[t + 1]
        inside = (col >= low - reach[t]) & (col < high + reach[t + 1])
        masks.append(jnp.where(inside, 1.0, 0.0))
        inside_ref[k + 1] = masks[-1]
        there = jnp.where(there, 1, 0)
        core = (col >= low) & (col < high) & (local_col >= 1) & (local_col <= LCW)
        cores.append(jnp.where(core, there.astype(F32), 0.0))

    for c in range(8):
        columns = 40 * j - 8 + 8 * iota((8, 128), 0) + c
        parts = []
        for k in range(3):
            t, there = around(j, k - 1)
            weight = blend_weight(columns, anchors[t], anchors[t + 1], reach[t], reach[t + 1])
            parts.append(weight * jnp.where(there, 1, 0).astype(F32))
        total = parts[0] + parts[1] + parts[2]
        keep = (iota((8, 128), 0) >= 1) & (iota((8, 128), 0) <= LCW)
        total = jnp.where(keep, total, 1.0)
        for k in range(3):
            blend_ref[3 * c + k] = parts[k] / total

    await_all(b1.at[pl.ds(1, 31)], rb1)
    totals = [jnp.sum(b1[8 * s : 8 * s + 8], axis=0) for s in range(3)]
    stats = decode(totals, float(2 * LCW * TILES * 8))

    def block(s):
        at = 16 * (2 - s)
        return normalize(projected[at : at + 16], stats[s][0], stats[s][1], gain[...], shift[...])

    now, before = block(0), block(1)
    first = now[0:8]
    before = [jnp.where(tm == 0, first, before[0:8]), jnp.where(tm == 0, first, before[8:16])]

    def taps_of(frames):
        seqs = [jnp.concatenate(frames[a : a + 2], axis=0).astype(BF) for a in range(3)]
        return [
            [
                dot(seqs[0], hw[3 * b + d])
                + dot(seqs[1], hw[9 + 3 * b + d])
                + dot(seqs[2], hw[18 + 3 * b + d])
                for d in range(3)
            ]
            for b in range(3)
        ]

    def rolled(v, by):
        return pltpu.roll(v.reshape(2, 8, 256), by % 8, 1).reshape(16, 256)

    def middles(taps):
        for r in range(3):
            if r == 0:
                q = [taps[1][d] + taps[2][d] for d in range(3)]
            elif r == 1:
                q = [taps[0][d] + taps[1][d] + taps[2][d] for d in range(3)]
            else:
                q = [taps[0][d] + taps[1][d] for d in range(3)]
            right = q[1] + q[2]
            left = q[0] + q[1]
            whole = left + q[2]
            for k in range(3):
                m = masks[k]
                yield k, r, 0, rolled(m * q[0], 1) + m * right
                yield k, r, 1, m * whole
                yield k, r, 2, m * left + rolled(m * q[2], -1)

    sums = jnp.zeros((8, 256), F32)
    squares = jnp.zeros((8, 256), F32)
    for k, r, p, value in middles(taps_of([*before, now[0:8], now[8:16]])):
        mid_ref[k * 9 + r * 3 + p, 16:32] = value
        times = (2.0 if r == 1 else 1.0) * (2.0 if p == 1 else 1.0)
        part = cores[k] * value
        square = part * value
        sums = sums + times * (part[0:8] + part[8:16])
        squares = squares + times * (square[0:8] + square[8:16])
    b2[0] = encode(jnp.sum(sums, axis=0, keepdims=True), jnp.sum(squares, axis=0, keepdims=True))
    for s, dy, dz, dx in everyone:
        send(
            b2.at[0], b2.at[64 * s + 8 * dy + dz * NX + dx], sb2, rb2,
            (tile_at((y + dy) % NY, (z + dz) % NZH, (x + dx) % NX), (tm + s) % NT),
        )

    oldest = block(2)
    oldest = [jnp.where(tm == 1, before[0], oldest[0:8]), jnp.where(tm == 1, before[0], oldest[8:16])]
    for k, r, p, value in middles(taps_of([*oldest, *before])):
        mid_ref[k * 9 + r * 3 + p, 0:16] = value

    await_all(wt.at[pl.ds(0, 3)], rw)
    for shard in ((tm + 2) % NT, (tm + 4) % NT, (tm + 6) % NT):
        send(wt.at[shard], wt.at[shard], ss, rs, sibling)

    await_all(wt.at[pl.ds(0, 4)], rs)

    def arrange(n, carry):
        for tap in range(9):
            for a in range(3):
                wc_ref[
                    pl.ds(pl.multiple_of(tap * 128 + n * 16, 16), 16), a * 256 : a * 256 + 256
                ] = wt[n, 9 * a + tap]
        return carry

    lax.fori_loop(0, NT, arrange, 0)

    await_all(b2.at[pl.ds(1, 127)], rb2)
    totals = [jnp.sum(b2[64 * s : 64 * s + 64], axis=0) for s in range(2)]
    stats = decode(totals, float(2 * 16 * LCW * TILES * 8))
    params_ref[0:1] = stats[1][0]
    params_ref[1:2] = stats[1][1]
    params_ref[2:3] = stats[0][0]
    params_ref[3:4] = stats[0][1]
    for part, sem in (
        (a1.at[pl.ds(1, 7)], sa1),
        (b1.at[pl.ds(1, 31)], sb1),
        (lbuf.at[pl.ds(0, 16)], sl),
        (wt.at[pl.ds(0, 3)], sw),
        (wt.at[pl.ds(0, 4)], ss),
        (b2.at[pl.ds(1, 127)], sb2),
    ):
        await_all(part, sem)


def back_kernel(
    mid, params, inside, blend, wc, out_ref, xs, prod, rows
):
    tm = lax.axis_index("tm")
    gain, shift, bias = params[4:5], params[5:6], params[6:7, 0:128]
    for k in range(3):
        keep = inside[k]
        for r in range(3):
            for p in range(3):
                values = mid[k * 9 + r * 3 + p]
                before = normalize(values[0:16], params[0:1], params[1:2], gain, shift)
                now = normalize(values[16:32], params[2:3], params[3:4], gain, shift)
                now = keep * now
                before = keep * before
                first = jnp.concatenate([now[0:8], now[0:8]], axis=0)
                before = jnp.where(tm == 0, first, before)
                at = (r * 3 + p) * 48 + k * 16
                xs[at : at + 16, 0:256] = before.astype(BF)
                xs[at : at + 16, 256:512] = jnp.concatenate([before[8:16], now[0:8]], axis=0).astype(BF)
                xs[at : at + 16, 512:768] = now.astype(BF)

    for n in range(0, 9, 2):
        many = min(2, 9 - n)
        result = lax.dot_general(
            xs[...], wc[n * 128 : (n + many) * 128], (((1,), (1,)), ((), ())), preferred_element_type=F32
        )
        for i in range(many):
            prod[n + i] = result[:, i * 128 : i * 128 + 128]

    def products(b, r, at):
        return [
            [prod[3 * b + d, (r * 3 + p) * 48 + at : (r * 3 + p) * 48 + at + 8] for p in range(3)]
            for d in range(3)
        ]

    for t in range(2):
        for k in range(3):
            at = k * 16 + t * 8
            across = {}
            for b in range(3):
                for r in range(3):
                    (a0, a1, a3), (b0, b1, b3), (c0, c1, c3) = products(b, r, at)
                    ab1, bc1 = a1 + b1, b1 + c1
                    across[b, r] = (
                        pltpu.roll(a3, 1, 0) + (b0 + c0),
                        (a0 + b0) + c1,
                        a0 + bc1,
                        ab1 + c1,
                        ab1 + c3,
                        a1 + (b3 + c3),
                        (a3 + b3) + pltpu.roll(c0, 7, 0),
                    )
            for c in range(7):
                (x0, x1, x3), (y0, y1, y3), (z0, z1, z3) = [
                    [across[b, r][c] for r in range(3)] for b in range(3)
                ]
                xy1, yz1 = x1 + y1, y1 + z1
                down = (
                    y0 + z0,
                    (x0 + y0) + z1,
                    x0 + yz1,
                    xy1 + z1,
                    xy1 + z3,
                    x1 + (y3 + z3),
                    x3 + y3,
                )
                for r in range(7):
                    value = (down[r] + bias).astype(BF).astype(F32)
                    for column in (3, 4) if c == 3 else (c if c < 3 else c + 1,):
                        place = pl.ds(column, 8, stride=8)
                        piece = value * blend[3 * column + k]
                        if k == 0:
                            rows[r, place, :] = piece
                        else:
                            rows[r, place, :] += piece
        for r in range(7):
            final = rows[r, 8:48].astype(BF)
            for big_row in (3, 4) if r == 3 else (r if r < 3 else r + 1,):
                out_ref[t, big_row] = final


def on_device(
    latent,
    proj_weight,
    first_gain,
    first_shift,
    half_weight,
    second_gain,
    second_shift,
    full_weight,
    full_bias,
    anchors,
    reach,
):
    lat = latent.transpose(1, 2, 3, 0, 4).reshape(LCW, 2, 16)
    shard = full_weight.transpose(0, 2, 1)
    any_space = pl.BlockSpec(memory_space=pl.ANY)
    vmem = pl.BlockSpec(memory_space=pltpu.VMEM)
    dma = pltpu.SemaphoreType.DMA
    held = pl.pallas_call(
        front_kernel,
        name="front",
        out_shape=(
            jax.ShapeDtypeStruct((27, 32, 256), F32),
            jax.ShapeDtypeStruct((8, 256), F32),
            jax.ShapeDtypeStruct((3, 16, 256), F32),
            jax.ShapeDtypeStruct((24, 8, 128), F32),
            jax.ShapeDtypeStruct((9 * 128, 768), BF),
        ),
        in_specs=[any_space] * 11,
        out_specs=(vmem,) * 5,
        scratch_shapes=[
            pltpu.VMEM((3 * (LCW + 2), 2, 16), BF),
            pltpu.VMEM((16, 256), BF),
            pltpu.VMEM((1, 256), F32),
            pltpu.VMEM((1, 256), F32),
            pltpu.VMEM((27, 256, 256), BF),
            pltpu.VMEM((NT, 27, 16, 256), BF),
            pltpu.SMEM((TILES + 1,), jnp.int32),
            pltpu.SMEM((TILES + 1,), jnp.int32),
            pltpu.VMEM((1, 256), F32),
            pltpu.VMEM((1, 256), F32),
            pltpu.VMEM((1, 128), F32),
            pltpu.VMEM((48, 16), F32),
            pltpu.VMEM((8, 1, 128), F32),
            pltpu.VMEM((32, 1, 128), F32),
            pltpu.VMEM((128, 1, 128), F32),
            dma((13,)),
            *[dma] * 12,
        ],
        compiler_params=pltpu.CompilerParams(
            collective_id=0, has_side_effects=True, vmem_limit_bytes=20 * 2**20
        ),
    )(
        *(
            pltpu.with_memory_space_constraint(v, pltpu.HBM)
            for v in (
                lat, proj_weight, first_gain.reshape(1, 256), first_shift.reshape(1, 256),
                half_weight, shard, anchors, reach,
                second_gain.reshape(1, 256), second_shift.reshape(1, 256), full_bias.reshape(1, 128),
            )
        )
    )
    out = pl.pallas_call(
        back_kernel,
        name="back",
        out_shape=jax.ShapeDtypeStruct((2, 8, 8 * LCW, 128), BF),
        in_specs=[vmem] * 5,
        out_specs=vmem,
        scratch_shapes=[
            pltpu.VMEM((432, 768), BF),
            pltpu.VMEM((9, 432, 128), F32),
            pltpu.VMEM((7, 64, 128), F32),
        ],
        compiler_params=pltpu.CompilerParams(vmem_limit_bytes=20 * 2**20),
    )(*held)
    return out[:, None]


def solution(mesh):
    return jax.shard_map(
        on_device,
        mesh=mesh,
        in_specs=(
            P("tm", "tile", None, None, None),
            P(),
            P(),
            P(),
            P(),
            P(),
            P(),
            P(None, None, "tm"),
            P(),
            P(),
            P(),
        ),
        out_specs=P("tm", "tile", None, None, None),
        check_vma=False,
    )
```

```python
import jax
import jax.numpy as jnp
from jax import lax
from jax.experimental import pallas as pl
from jax.experimental.pallas import tpu as pltpu
from jax.sharding import PartitionSpec as P

GROUPS = 32
NX, NZH, NY, NT = 4, 2, 8, 8
TILES = NX * NZH * NY
LCW = 5
BF = jnp.bfloat16
F32 = jnp.float32
MESH = pl.DeviceIdType.MESH


def dot(a, b):
    return jnp.dot(a, b, preferred_element_type=F32)


def exact_dot(x, ones):
    high = x.astype(BF).astype(F32)
    rest = x - high
    middle = rest.astype(BF).astype(F32)
    parts = jnp.concatenate([high, middle, rest - middle, jnp.zeros_like(x)], axis=0).astype(BF)
    y = dot(parts, ones)
    return y[0:8] + y[8:16] + y[16:24]


def iota(shape, dim):
    return lax.broadcasted_iota(jnp.int32, shape, dim)


def group_ones(shape, channel_dim):
    channel, lane = iota(shape, channel_dim), iota(shape, 1 - channel_dim)
    return jnp.where(((channel >> 3) == (lane & 31)) & (lane < 64), 1.0, 0.0).astype(BF)


def encode(sums, squares, ones):
    row = iota((8, 256), 0)
    coded = exact_dot(jnp.where(row == 0, sums, jnp.where(row == 1, squares, 0.0)), ones)
    return jnp.where(iota((1, 128), 1) < 32, coded[0:1], coded[1:2])


def decode(totals, count, ones):
    row, place = iota((8, 128), 0), iota((8, 128), 1)
    stacked = jnp.zeros((8, 128), F32)
    for i, total in enumerate(totals):
        stacked = jnp.where((row == 2 * i) & (place < 32), total, stacked)
        stacked = jnp.where((row == 2 * i + 1) & (place >= 32), total, stacked)
    wide = exact_dot(stacked, ones)
    result = []
    for i in range(len(totals)):
        mean = wide[2 * i : 2 * i + 1] * (1.0 / count)
        variance = wide[2 * i + 1 : 2 * i + 2] * (1.0 / count) - mean * mean
        result.append((mean, lax.rsqrt(variance + 1e-06)))
    return result


def normalize(values, mean, scale, gain, shift):
    v = gain * (values - mean) * scale + shift
    half = 0.5 * v
    return half + half * jnp.tanh(half)


def tile_at(y, z, x):
    return y * (NZH * NX) + z * NX + x


def around(j, k):
    other = j + k
    return jnp.clip(other, 0, TILES - 1), (other >= 0) & (other < TILES)


def blend_weight(columns, low, high, low_reach, high_reach):
    left_edge, right_edge = 8 * low, 8 * high
    left_reach, right_reach = 8 * low_reach, 8 * high_reach
    place = columns.astype(F32)
    rising = jnp.clip(
        (place - (left_edge - left_reach).astype(F32) + 0.5)
        / jnp.maximum(2 * left_reach, 1).astype(F32),
        0.0,
        1.0,
    )
    rising = jnp.where(left_reach > 0, rising, jnp.where(columns >= left_edge, 1.0, 0.0))
    falling = jnp.clip(
        ((right_edge + right_reach).astype(F32) - place - 0.5)
        / jnp.maximum(2 * right_reach, 1).astype(F32),
        0.0,
        1.0,
    )
    falling = jnp.where(right_reach > 0, falling, jnp.where(columns < right_edge, 1.0, 0.0))
    return jnp.minimum(rising, falling)


def front_kernel(
    lat_hbm, wp_hbm, gain_hbm, shift_hbm, hw_hbm, fw_hbm, anchors_hbm, reach_hbm,
    gain2_hbm, shift2_hbm, bias_hbm,
    mid_ref, params_ref, inside_ref, blend_ref, wc_ref,
    lbuf, wp, gain, shift, hw, wt, anchors, reach, gain2, shift2, bias, fl, enc, dec, a1, b1, b2,
    local_sem, sa1, ra1, sb1, rb1, sb2, rb2, sl, rl, sw, rw, ss, rs,
):
    j = lax.axis_index("tile")
    tm = lax.axis_index("tm")
    y, z, x = j // (NZH * NX), (j // NX) % NZH, j % NX
    zl = tm // 2

    loads = [
        pltpu.make_async_copy(src, dst, local_sem.at[i])
        for i, (src, dst) in enumerate(
            (
                (lat_hbm, lbuf.at[pl.ds(1, LCW)]),
                (wp_hbm, wp),
                (fw_hbm, wt.at[tm]),
                (anchors_hbm, anchors),
                (reach_hbm, reach),
                (gain_hbm, gain),
                (shift_hbm, shift),
                (gain2_hbm, gain2),
                (shift2_hbm, shift2),
                (bias_hbm, bias),
                (hw_hbm.at[pl.ds(0, 9)], hw.at[pl.ds(0, 9)]),
                (hw_hbm.at[pl.ds(9, 9)], hw.at[pl.ds(9, 9)]),
                (hw_hbm.at[pl.ds(18, 9)], hw.at[pl.ds(18, 9)]),
            )
        )
    ]
    loads[0].start()
    loads[1].start()

    column = [(tile_at((y + d) % NY, z, x), tm) for d in range(NY)]
    shifts = (0, 1, 2, -1)
    plane = [(i, dz, dx) for i in range(4) for dz in range(NZH) for dx in range(NX)][1:]
    plane.sort(key=lambda p: -(4 * p[1] + min(p[2], NX - p[2])))
    everyone = [
        (s, dy, dz, dx) for s in range(2) for dy in range(NY) for dz in range(NZH) for dx in range(NX)
    ][1:]
    everyone.sort(key=lambda p: -(min(p[1], NY - p[1]) + 4 * p[2] + min(p[3], NX - p[3])))

    def plane_at(sign, i, dz, dx):
        return (
            tile_at(y, (z + dz) % NZH, (x + sign * dx + NX) % NX),
            (tm + sign * shifts[i] + NT) % NT,
        )

    def chip_at(step):
        far = (zl + step + 4) // 4
        return (tile_at(y, (z + far + 1) % NZH, x), (tm + 2 * step + NT) % NT)

    sibling = (j, tm + 1 - 2 * (tm % 2))
    chips = [chip_at(1), chip_at(-1), chip_at(2), chip_at(-2)]

    barrier = pltpu.get_barrier_semaphore()
    greeted = []
    for s in range(3):
        greeted.append(((j + 1) % TILES, (tm - s + NT) % NT))
        greeted.append(((j + TILES - 1) % TILES, (tm - s + NT) % NT))
    greeted += [plane_at(-1, *p) for p in plane] + column[1:] + chips + [sibling]
    for peer in greeted:
        pl.semaphore_signal(barrier, inc=1, device_id=peer, device_id_type=MESH)
    for load in loads[2:]:
        load.start()
    enc[...] = group_ones((256, 128), 0)
    dec[...] = group_ones((128, 256), 1)

    fl[...] = jnp.zeros_like(fl)
    loads[0].wait()
    loads[1].wait()
    for c in range(LCW):
        fl[pl.ds(32 + 1 + c, 2, stride=8), :] = lbuf[1 + c].astype(F32)
    own = dot(fl[32:48].astype(BF), wp[...])
    a1[0] = encode(jnp.sum(own, axis=0, keepdims=True), jnp.sum(own * own, axis=0, keepdims=True), enc[...])

    pl.semaphore_wait(barrier, len(greeted))

    def send(src, dst, send_sem, recv_sem, peer):
        pltpu.make_async_remote_copy(
            src_ref=src, dst_ref=dst, send_sem=send_sem, recv_sem=recv_sem,
            device_id=peer, device_id_type=MESH,
        ).start()

    def await_all(part, sem):
        pltpu.make_async_copy(part, part, sem).wait()

    def send_column(buf, s_sem, r_sem):
        for d in (4, 3, 5, 2, 6, 1, 7):
            send(buf.at[0], buf.at[d], s_sem, r_sem, column[d])

    send_column(a1, sa1, ra1)
    for s in range(3):
        first = s * (LCW + 2)
        for i, (src, dst, tile) in enumerate(
            (
                (lbuf.at[LCW], lbuf.at[first], (j + 1) % TILES),
                (lbuf.at[1], lbuf.at[first + LCW + 1], (j + TILES - 1) % TILES),
                (lbuf.at[pl.ds(1, LCW)], lbuf.at[pl.ds(first + 1, LCW)], j),
            )
        ):
            if i == 2 and s == 0:
                continue
            send(src, dst, sl, rl, (tile, (tm + s) % NT))
    loads[2].wait()
    send(wt.at[tm], wt.at[tm], ss, rs, sibling)

    await_all(a1.at[pl.ds(1, 7)], ra1)
    b1[0] = jnp.sum(a1[...], axis=0)
    for i, dz, dx in plane:
        send(b1.at[0], b1.at[8 * i + dz * NX + dx], sb1, rb1, plane_at(1, i, dz, dx))

    half = 14
    send(wt.at[tm], wt.at[tm], sw, rw, chips[0])
    send(wt.at[tm], wt.at[tm], sw, rw, chips[1])
    for first, many, chip in ((0, half, chips[2]), (half, 27 - half, chips[3])):
        part = wt.at[tm, pl.ds(first, many)]
        send(part, part, sw, rw, chip)

    await_all(lbuf.at[pl.ds(0, 16)], rl)
    for s in range(3):
        for c in range(LCW + 2):
            fl[pl.ds(16 * (2 - s) + c, 2, stride=8), :] = lbuf[s * (LCW + 2) + c].astype(F32)
    projected = dot(fl[...].astype(BF), wp[...])
    for load in loads[3:]:
        load.wait()

    params_ref[4:5, 0:128] = bias[...]
    col = 5 * j - 1 + (iota((16, 256), 0) & 7)
    local_col = iota((16, 256), 0) & 7
    masks, cores = [], []
    for k in (-1, 0, 1):
        t, there = around(j, k)
        low, high = anchors[t], anchors[t + 1]
        inside = (col >= low - reach[t]) & (col < high + reach[t + 1])
        masks.append(jnp.where(inside, 1.0, 0.0))
        inside_ref[k + 1] = masks[-1]
        there = jnp.where(there, 1, 0)
        core = (col >= low) & (col < high) & (local_col >= 1) & (local_col <= LCW)
        cores.append(jnp.where(core, there.astype(F32), 0.0))

    for c in range(8):
        columns = 40 * j - 8 + 8 * iota((8, 128), 0) + c
        parts = []
        for k in range(3):
            t, there = around(j, k - 1)
            weight = blend_weight(columns, anchors[t], anchors[t + 1], reach[t], reach[t + 1])
            parts.append(weight * jnp.where(there, 1, 0).astype(F32))
        total = parts[0] + parts[1] + parts[2]
        keep = (iota((8, 128), 0) >= 1) & (iota((8, 128), 0) <= LCW)
        total = jnp.where(keep, total, 1.0)
        for k in range(3):
            blend_ref[3 * c + k] = parts[k] / total

    await_all(b1.at[pl.ds(1, 31)], rb1)
    totals = [jnp.sum(b1[8 * s : 8 * s + 8], axis=0) for s in range(3)]
    stats = decode(totals, float(2 * LCW * TILES * 8), dec[...])

    def block(s):
        at = 16 * (2 - s)
        return normalize(projected[at : at + 16], stats[s][0], stats[s][1], gain[...], shift[...])

    now, before = block(0), block(1)
    first = now[0:8]
    before = [jnp.where(tm == 0, first, before[0:8]), jnp.where(tm == 0, first, before[8:16])]

    def taps_of(frames):
        seqs = [jnp.concatenate(frames[a : a + 2], axis=0).astype(BF) for a in range(3)]
        return [
            [
                dot(seqs[0], hw[3 * b + d])
                + dot(seqs[1], hw[9 + 3 * b + d])
                + dot(seqs[2], hw[18 + 3 * b + d])
                for d in range(3)
            ]
            for b in range(3)
        ]

    def rolled(v, by):
        return pltpu.roll(v.reshape(2, 8, 256), by % 8, 1).reshape(16, 256)

    def middles(taps):
        for r in range(3):
            if r == 0:
                q = [taps[1][d] + taps[2][d] for d in range(3)]
            elif r == 1:
                q = [taps[0][d] + taps[1][d] + taps[2][d] for d in range(3)]
            else:
                q = [taps[0][d] + taps[1][d] for d in range(3)]
            right = q[1] + q[2]
            left = q[0] + q[1]
            whole = left + q[2]
            for k in range(3):
                m = masks[k]
                yield k, r, 0, rolled(m * q[0], 1) + m * right
                yield k, r, 1, m * whole
                yield k, r, 2, m * left + rolled(m * q[2], -1)

    sums = jnp.zeros((8, 256), F32)
    squares = jnp.zeros((8, 256), F32)
    for k, r, p, value in middles(taps_of([*before, now[0:8], now[8:16]])):
        mid_ref[k * 9 + r * 3 + p, 16:32] = value
        times = (2.0 if r == 1 else 1.0) * (2.0 if p == 1 else 1.0)
        part = cores[k] * value
        square = part * value
        sums = sums + times * (part[0:8] + part[8:16])
        squares = squares + times * (square[0:8] + square[8:16])
    b2[0] = encode(jnp.sum(sums, axis=0, keepdims=True), jnp.sum(squares, axis=0, keepdims=True), enc[...])
    for s, dy, dz, dx in everyone:
        send(
            b2.at[0], b2.at[64 * s + 8 * dy + dz * NX + dx], sb2, rb2,
            (tile_at((y + dy) % NY, (z + dz) % NZH, (x + dx) % NX), (tm + s) % NT),
        )

    oldest = block(2)
    oldest = [jnp.where(tm == 1, before[0], oldest[0:8]), jnp.where(tm == 1, before[0], oldest[8:16])]
    for k, r, p, value in middles(taps_of([*oldest, *before])):
        i = k * 9 + r * 3 + p
        start = mid_ref[i, 16:24]
        mid_ref[i, 0:8] = jnp.where(tm == 0, start, value[0:8])
        mid_ref[i, 8:16] = jnp.where(tm == 0, start, value[8:16])

    await_all(wt.at[pl.ds(0, 3)], rw)
    for shard in ((tm + 2) % NT, (tm + 4) % NT, (tm + 6) % NT):
        send(wt.at[shard], wt.at[shard], ss, rs, sibling)

    await_all(wt.at[pl.ds(0, 4)], rs)

    def arrange(n, carry):
        for tap in range(9):
            for a in range(3):
                wc_ref[
                    pl.ds(pl.multiple_of(tap * 128 + n * 16, 16), 16), a * 256 : a * 256 + 256
                ] = wt[n, 9 * a + tap]
        return carry

    lax.fori_loop(0, NT, arrange, 0)

    for part, sem in (
        (a1.at[pl.ds(1, 7)], sa1),
        (b1.at[pl.ds(1, 31)], sb1),
        (lbuf.at[pl.ds(0, 16)], sl),
        (wt.at[pl.ds(0, 3)], sw),
        (wt.at[pl.ds(0, 4)], ss),
        (b2.at[pl.ds(1, 127)], sb2),
    ):
        await_all(part, sem)
    await_all(b2.at[pl.ds(1, 127)], rb2)
    totals = [jnp.sum(b2[64 * s : 64 * s + 64], axis=0) for s in range(2)]
    stats = decode(totals, float(2 * 16 * LCW * TILES * 8), dec[...])
    for i, s in enumerate((1, 0)):
        alpha = 0.5 * gain2[...] * stats[s][1]
        beta = 0.5 * shift2[...] - stats[s][0] * alpha
        if s == 0:
            params_ref[2:3] = alpha
            params_ref[3:4] = beta
            alpha_before, beta_before = (
                jnp.where(tm == 0, now_, before_) for now_, before_ in ((alpha, last[0]), (beta, last[1]))
            )
            params_ref[0:1] = alpha_before
            params_ref[1:2] = beta_before
        last = alpha, beta


def back_kernel(
    mid, params, inside, blend, wc, out_ref, xs, prod, rows
):
    bias = params[4:5, 0:128]
    for r in range(3):
        for p in range(3):
            for k in range(3):
                values = mid[k * 9 + r * 3 + p]
                keep = inside[k]

                def activate(v, row):
                    half = v * params[row : row + 1] + params[row + 1 : row + 2]
                    return keep * (half + half * jnp.tanh(half))

                before = activate(values[0:16], 0)
                now = activate(values[16:32], 2)
                at = (r * 3 + p) * 48 + k * 16
                xs[at : at + 16, 0:256] = before.astype(BF)
                xs[at : at + 16, 256:512] = jnp.concatenate([before[8:16], now[0:8]], axis=0).astype(BF)
                xs[at : at + 16, 512:768] = now.astype(BF)

    for n in range(0, 9, 2):
        many = min(2, 9 - n)
        result = lax.dot_general(
            xs[...], wc[n * 128 : (n + many) * 128], (((1,), (1,)), ((), ())), preferred_element_type=F32
        )
        for i in range(many):
            prod[n + i] = result[:, i * 128 : i * 128 + 128]

    def products(b, r, at):
        return [
            [prod[3 * b + d, (r * 3 + p) * 48 + at : (r * 3 + p) * 48 + at + 8] for p in range(3)]
            for d in range(3)
        ]

    for t in range(2):
        across = {}
        for k in range(3):
            at = k * 16 + t * 8
            for b in range(3):
                for r in range(3):
                    (a0, a1, a3), (b0, b1, b3), (c0, c1, c3) = products(b, r, at)
                    bc1 = b1 + c1
                    ab1 = a1 + b1
                    across[k, b, r] = (
                        pltpu.roll(a3, 1, 0) + (b0 + c0),
                        (a0 + b0) + c1,
                        a0 + bc1,
                        ab1 + c1,
                        ab1 + c3,
                        a1 + (b3 + c3),
                        (a3 + b3) + pltpu.roll(c0, 7, 0),
                    )
        for c in range(7):
            columns = (3, 4) if c == 3 else (c if c < 3 else c + 1,)
            totals = [[None] * 7 for _ in columns]
            for k in range(3):
                (x0, x1, x3), (y0, y1, y3), (z0, z1, z3) = [
                    [across[k, b, r][c] for r in range(3)] for b in range(3)
                ]
                xy1, yz1 = x1 + y1, y1 + z1
                down = (
                    y0 + z0,
                    (x0 + y0) + z1,
                    x0 + yz1,
                    xy1 + z1,
                    xy1 + z3,
                    x1 + (y3 + z3),
                    x3 + y3,
                )
                for r in range(7):
                    value = (down[r] + bias).astype(BF).astype(F32)
                    for i, column in enumerate(columns):
                        piece = value * blend[3 * column + k]
                        totals[i][r] = piece if k == 0 else totals[i][r] + piece
            for i, column in enumerate(columns):
                for r in range(7):
                    rows[r, pl.ds(column, 8, stride=8), :] = totals[i][r]
        for r in range(7):
            final = rows[r, 8:48].astype(BF)
            for big_row in (3, 4) if r == 3 else (r if r < 3 else r + 1,):
                out_ref[t, big_row] = final


def on_device(
    latent,
    proj_weight,
    first_gain,
    first_shift,
    half_weight,
    second_gain,
    second_shift,
    full_weight,
    full_bias,
    anchors,
    reach,
):
    lat = latent.transpose(1, 2, 3, 0, 4).reshape(LCW, 2, 16)
    shard = full_weight.transpose(0, 2, 1)
    any_space = pl.BlockSpec(memory_space=pl.ANY)
    vmem = pl.BlockSpec(memory_space=pltpu.VMEM)
    dma = pltpu.SemaphoreType.DMA
    held = pl.pallas_call(
        front_kernel,
        name="front",
        out_shape=(
            jax.ShapeDtypeStruct((27, 32, 256), F32),
            jax.ShapeDtypeStruct((8, 256), F32),
            jax.ShapeDtypeStruct((3, 16, 256), F32),
            jax.ShapeDtypeStruct((24, 8, 128), F32),
            jax.ShapeDtypeStruct((9 * 128, 768), BF),
        ),
        in_specs=[any_space] * 11,
        out_specs=(vmem,) * 5,
        scratch_shapes=[
            pltpu.VMEM((3 * (LCW + 2), 2, 16), BF),
            pltpu.VMEM((16, 256), BF),
            pltpu.VMEM((1, 256), F32),
            pltpu.VMEM((1, 256), F32),
            pltpu.VMEM((27, 256, 256), BF),
            pltpu.VMEM((NT, 27, 16, 256), BF),
            pltpu.SMEM((TILES + 1,), jnp.int32),
            pltpu.SMEM((TILES + 1,), jnp.int32),
            pltpu.VMEM((1, 256), F32),
            pltpu.VMEM((1, 256), F32),
            pltpu.VMEM((1, 128), F32),
            pltpu.VMEM((48, 16), F32),
            pltpu.VMEM((256, 128), BF),
            pltpu.VMEM((128, 256), BF),
            pltpu.VMEM((8, 1, 128), F32),
            pltpu.VMEM((32, 1, 128), F32),
            pltpu.VMEM((128, 1, 128), F32),
            dma((13,)),
            *[dma] * 12,
        ],
        compiler_params=pltpu.CompilerParams(
            collective_id=0, has_side_effects=True, vmem_limit_bytes=20 * 2**20
        ),
    )(
        *(
            pltpu.with_memory_space_constraint(v, pltpu.HBM)
            for v in (
                lat, proj_weight, first_gain.reshape(1, 256), first_shift.reshape(1, 256),
                half_weight, shard, anchors, reach,
                second_gain.reshape(1, 256), second_shift.reshape(1, 256), full_bias.reshape(1, 128),
            )
        )
    )
    out = pl.pallas_call(
        back_kernel,
        name="back",
        out_shape=jax.ShapeDtypeStruct((2, 8, 8 * LCW, 128), BF),
        in_specs=[vmem] * 5,
        out_specs=vmem,
        scratch_shapes=[
            pltpu.VMEM((432, 768), BF),
            pltpu.VMEM((9, 432, 128), F32),
            pltpu.VMEM((7, 64, 128), F32),
        ],
        compiler_params=pltpu.CompilerParams(vmem_limit_bytes=20 * 2**20),
    )(*held)
    return out[:, None]


def solution(mesh):
    return jax.shard_map(
        on_device,
        mesh=mesh,
        in_specs=(
            P("tm", "tile", None, None, None),
            P(),
            P(),
            P(),
            P(),
            P(),
            P(),
            P(None, None, "tm"),
            P(),
            P(),
            P(),
        ),
        out_specs=P("tm", "tile", None, None, None),
        check_vma=False,
    )
```

```python
import jax
import jax.numpy as jnp
from jax import lax
from jax.experimental import pallas as pl
from jax.experimental.pallas import tpu as pltpu
from jax.sharding import PartitionSpec as P

GROUPS = 32
NX, NZH, NY, NT = 4, 2, 8, 8
TILES = NX * NZH * NY
LCW = 5
BF = jnp.bfloat16
F32 = jnp.float32
MESH = pl.DeviceIdType.MESH


def dot(a, b):
    return jnp.dot(a, b, preferred_element_type=F32)


def exact_dot(x, ones):
    high = x.astype(BF).astype(F32)
    rest = x - high
    middle = rest.astype(BF).astype(F32)
    parts = jnp.concatenate([high, middle, rest - middle, jnp.zeros_like(x)], axis=0).astype(BF)
    y = dot(parts, ones)
    return y[0:8] + y[8:16] + y[16:24]


def iota(shape, dim):
    return lax.broadcasted_iota(jnp.int32, shape, dim)


def group_ones():
    channel, lane = iota((256, 128), 0), iota((256, 128), 1)
    return jnp.where(((channel >> 3) == (lane & 31)) & (lane < 64), 1.0, 0.0).astype(BF)


def encode(sums, squares, ones):
    row = iota((8, 256), 0)
    coded = exact_dot(jnp.where(row == 0, sums, jnp.where(row == 1, squares, 0.0)), ones)
    return jnp.where(iota((1, 128), 1) < 32, coded[0:1], coded[1:2])


def decode(totals, count):
    row, lane = iota((8, 128), 0), iota((8, 128), 1)
    stacked = jnp.zeros((8, 128), F32)
    for i, total in enumerate(totals):
        stacked = jnp.where(row == i, total, stacked)

    def spread(first):
        parts = [
            jnp.take_along_axis(stacked, first + half + (lane >> 3), axis=1, mode="promise_in_bounds")
            for half in (0, 16)
        ]
        return jnp.concatenate(parts, axis=1) * (1.0 / count)

    mean = spread(0)
    scale = lax.rsqrt(spread(32) - mean * mean + 1e-06)
    return [(mean[i : i + 1], scale[i : i + 1]) for i in range(len(totals))]


def normalize(values, mean, scale, gain, shift):
    v = gain * (values - mean) * scale + shift
    half = 0.5 * v
    return half + half * jnp.tanh(half)


def tile_at(y, z, x):
    return y * (NZH * NX) + z * NX + x


def around(j, k):
    other = j + k
    return jnp.clip(other, 0, TILES - 1), (other >= 0) & (other < TILES)


def blend_weight(columns, low, high, low_reach, high_reach):
    left_edge, right_edge = 8 * low, 8 * high
    left_reach, right_reach = 8 * low_reach, 8 * high_reach
    place = columns.astype(F32)
    rising = jnp.clip(
        (place - (left_edge - left_reach).astype(F32) + 0.5)
        / jnp.maximum(2 * left_reach, 1).astype(F32),
        0.0,
        1.0,
    )
    rising = jnp.where(left_reach > 0, rising, jnp.where(columns >= left_edge, 1.0, 0.0))
    falling = jnp.clip(
        ((right_edge + right_reach).astype(F32) - place - 0.5)
        / jnp.maximum(2 * right_reach, 1).astype(F32),
        0.0,
        1.0,
    )
    falling = jnp.where(right_reach > 0, falling, jnp.where(columns < right_edge, 1.0, 0.0))
    return jnp.minimum(rising, falling)


def front_kernel(
    lat_hbm, wp_hbm, gain_hbm, shift_hbm, hw_hbm, fw_hbm, anchors_hbm, reach_hbm,
    gain2_hbm, shift2_hbm, bias_hbm,
    mid_ref, params_ref, inside_ref, blend_ref, wc_ref,
    lbuf, wp, gain, shift, hw, wt, anchors, reach, gain2, shift2, bias, fl, enc, a1, b1, b2,
    local_sem, sa1, ra1, sb1, rb1, sb2, rb2, sl, rl, sw, rw, ss, rs,
):
    j = lax.axis_index("tile")
    tm = lax.axis_index("tm")
    y, z, x = j // (NZH * NX), (j // NX) % NZH, j % NX
    zl = tm // 2

    loads = [
        pltpu.make_async_copy(src, dst, local_sem.at[i])
        for i, (src, dst) in enumerate(
            (
                (lat_hbm, lbuf.at[pl.ds(1, LCW)]),
                (wp_hbm, wp),
                (fw_hbm, wt.at[tm]),
                (anchors_hbm, anchors),
                (reach_hbm, reach),
                (gain_hbm, gain),
                (shift_hbm, shift),
                (gain2_hbm, gain2),
                (shift2_hbm, shift2),
                (bias_hbm, bias),
                (hw_hbm.at[pl.ds(0, 9)], hw.at[pl.ds(0, 9)]),
                (hw_hbm.at[pl.ds(9, 9)], hw.at[pl.ds(9, 9)]),
                (hw_hbm.at[pl.ds(18, 9)], hw.at[pl.ds(18, 9)]),
            )
        )
    ]
    loads[0].start()
    loads[1].start()

    column = [(tile_at((y + d) % NY, z, x), tm) for d in range(NY)]
    shifts = (0, 1, 2, -1)
    plane = [(i, dz, dx) for i in range(4) for dz in range(NZH) for dx in range(NX)][1:]
    plane.sort(key=lambda p: -(4 * p[1] + min(p[2], NX - p[2])))
    everyone = [
        (s, dy, dz, dx) for s in range(2) for dy in range(NY) for dz in range(NZH) for dx in range(NX)
    ][1:]
    everyone.sort(key=lambda p: -(min(p[1], NY - p[1]) + 4 * p[2] + min(p[3], NX - p[3])))

    def plane_at(sign, i, dz, dx):
        return (
            tile_at(y, (z + dz) % NZH, (x + sign * dx + NX) % NX),
            (tm + sign * shifts[i] + NT) % NT,
        )

    def chip_at(step):
        far = (zl + step + 4) // 4
        return (tile_at(y, (z + far + 1) % NZH, x), (tm + 2 * step + NT) % NT)

    sibling = (j, tm + 1 - 2 * (tm % 2))
    chips = [chip_at(1), chip_at(-1), chip_at(2), chip_at(-2)]

    barrier = pltpu.get_barrier_semaphore()
    greeted = [column[d] for d in (4, 3, 5, 2, 6, 1, 7)]
    for s in range(3):
        greeted.append(((j + 1) % TILES, (tm - s + NT) % NT))
        greeted.append(((j + TILES - 1) % TILES, (tm - s + NT) % NT))
    greeted += [plane_at(-1, *p) for p in plane] + chips + [sibling]
    for peer in greeted:
        pl.semaphore_signal(barrier, inc=1, device_id=peer, device_id_type=MESH)
    for load in loads[2:]:
        load.start()
    enc[...] = group_ones()

    fl[...] = jnp.zeros_like(fl)
    loads[0].wait()
    loads[1].wait()
    for c in range(LCW):
        fl[pl.ds(32 + 1 + c, 2, stride=8), :] = lbuf[1 + c].astype(F32)
    own = dot(fl[32:48].astype(BF), wp[...])
    a1[0] = encode(jnp.sum(own, axis=0, keepdims=True), jnp.sum(own * own, axis=0, keepdims=True), enc[...])

    pl.semaphore_wait(barrier, len(greeted))

    def send(src, dst, send_sem, recv_sem, peer):
        pltpu.make_async_remote_copy(
            src_ref=src, dst_ref=dst, send_sem=send_sem, recv_sem=recv_sem,
            device_id=peer, device_id_type=MESH,
        ).start()

    def await_all(part, sem):
        pltpu.make_async_copy(part, part, sem).wait()

    def send_column(buf, s_sem, r_sem):
        for d in (4, 3, 5, 2, 6, 1, 7):
            send(buf.at[0], buf.at[d], s_sem, r_sem, column[d])

    send_column(a1, sa1, ra1)
    for s in range(3):
        first = s * (LCW + 2)
        for i, (src, dst, tile) in enumerate(
            (
                (lbuf.at[LCW], lbuf.at[first], (j + 1) % TILES),
                (lbuf.at[1], lbuf.at[first + LCW + 1], (j + TILES - 1) % TILES),
                (lbuf.at[pl.ds(1, LCW)], lbuf.at[pl.ds(first + 1, LCW)], j),
            )
        ):
            if i == 2 and s == 0:
                continue
            send(src, dst, sl, rl, (tile, (tm + s) % NT))
    loads[2].wait()
    send(wt.at[tm], wt.at[tm], ss, rs, sibling)

    await_all(a1.at[pl.ds(1, 7)], ra1)
    b1[0] = jnp.sum(a1[...], axis=0)
    for i, dz, dx in plane:
        send(b1.at[0], b1.at[8 * i + dz * NX + dx], sb1, rb1, plane_at(1, i, dz, dx))

    half = 14
    send(wt.at[tm], wt.at[tm], sw, rw, chips[0])
    send(wt.at[tm], wt.at[tm], sw, rw, chips[1])
    for first, many, chip in ((0, half, chips[2]), (half, 27 - half, chips[3])):
        part = wt.at[tm, pl.ds(first, many)]
        send(part, part, sw, rw, chip)

    await_all(lbuf.at[pl.ds(0, 16)], rl)
    for s in range(3):
        for c in range(LCW + 2):
            fl[pl.ds(16 * (2 - s) + c, 2, stride=8), :] = lbuf[s * (LCW + 2) + c].astype(F32)
    projected = dot(fl[...].astype(BF), wp[...])
    for load in loads[3:]:
        load.wait()

    params_ref[4:5, 0:128] = bias[...]
    col = 5 * j - 1 + (iota((16, 256), 0) & 7)
    local_col = iota((16, 256), 0) & 7
    masks, cores = [], []
    for k in (-1, 0, 1):
        t, there = around(j, k)
        low, high = anchors[t], anchors[t + 1]
        inside = (col >= low - reach[t]) & (col < high + reach[t + 1])
        masks.append(jnp.where(inside, 1.0, 0.0))
        inside_ref[k + 1] = masks[-1]
        there = jnp.where(there, 1, 0)
        core = (col >= low) & (col < high) & (local_col >= 1) & (local_col <= LCW)
        cores.append(jnp.where(core, there.astype(F32), 0.0))

    for c in range(8):
        columns = 40 * j - 8 + 8 * iota((8, 128), 0) + c
        parts = []
        for k in range(3):
            t, there = around(j, k - 1)
            weight = blend_weight(columns, anchors[t], anchors[t + 1], reach[t], reach[t + 1])
            parts.append(weight * jnp.where(there, 1, 0).astype(F32))
        total = parts[0] + parts[1] + parts[2]
        keep = (iota((8, 128), 0) >= 1) & (iota((8, 128), 0) <= LCW)
        total = jnp.where(keep, total, 1.0)
        for k in range(3):
            blend_ref[3 * c + k] = parts[k] / total

    await_all(b1.at[pl.ds(1, 31)], rb1)
    totals = [jnp.sum(b1[8 * s : 8 * s + 8], axis=0) for s in range(3)]
    stats = decode(totals, float(2 * LCW * TILES * 8))

    def block(s):
        at = 16 * (2 - s)
        return normalize(projected[at : at + 16], stats[s][0], stats[s][1], gain[...], shift[...])

    now, before = block(0), block(1)
    first = now[0:8]
    before = [jnp.where(tm == 0, first, before[0:8]), jnp.where(tm == 0, first, before[8:16])]

    def taps_of(frames):
        seqs = [jnp.concatenate(frames[a : a + 2], axis=0).astype(BF) for a in range(3)]
        return [
            [
                dot(seqs[0], hw[3 * b + d])
                + dot(seqs[1], hw[9 + 3 * b + d])
                + dot(seqs[2], hw[18 + 3 * b + d])
                for d in range(3)
            ]
            for b in range(3)
        ]

    def rolled(v, by):
        return pltpu.roll(v.reshape(2, 8, 256), by % 8, 1).reshape(16, 256)

    def middles(taps):
        for r in range(3):
            if r == 0:
                q = [taps[1][d] + taps[2][d] for d in range(3)]
            elif r == 1:
                q = [taps[0][d] + taps[1][d] + taps[2][d] for d in range(3)]
            else:
                q = [taps[0][d] + taps[1][d] for d in range(3)]
            right = q[1] + q[2]
            left = q[0] + q[1]
            whole = left + q[2]
            for k in range(3):
                m = masks[k]
                yield k, r, 0, rolled(m * q[0], 1) + m * right
                yield k, r, 1, m * whole
                yield k, r, 2, m * left + rolled(m * q[2], -1)

    sums = jnp.zeros((8, 256), F32)
    squares = jnp.zeros((8, 256), F32)
    for k, r, p, value in middles(taps_of([*before, now[0:8], now[8:16]])):
        mid_ref[k * 9 + r * 3 + p, 16:32] = value
        times = (2.0 if r == 1 else 1.0) * (2.0 if p == 1 else 1.0)
        part = cores[k] * value
        square = part * value
        sums = sums + times * (part[0:8] + part[8:16])
        squares = squares + times * (square[0:8] + square[8:16])
    b2[0] = encode(jnp.sum(sums, axis=0, keepdims=True), jnp.sum(squares, axis=0, keepdims=True), enc[...])
    for s, dy, dz, dx in everyone:
        send(
            b2.at[0], b2.at[64 * s + 8 * dy + dz * NX + dx], sb2, rb2,
            (tile_at((y + dy) % NY, (z + dz) % NZH, (x + dx) % NX), (tm + s) % NT),
        )

    oldest = block(2)
    oldest = [jnp.where(tm == 1, before[0], oldest[0:8]), jnp.where(tm == 1, before[0], oldest[8:16])]
    for k, r, p, value in middles(taps_of([*oldest, *before])):
        i = k * 9 + r * 3 + p
        start = mid_ref[i, 16:24]
        mid_ref[i, 0:8] = jnp.where(tm == 0, start, value[0:8])
        mid_ref[i, 8:16] = jnp.where(tm == 0, start, value[8:16])

    await_all(wt.at[pl.ds(0, 3)], rw)
    for shard in ((tm + 2) % NT, (tm + 4) % NT, (tm + 6) % NT):
        send(wt.at[shard], wt.at[shard], ss, rs, sibling)

    await_all(wt.at[pl.ds(0, 4)], rs)

    def arrange(n, carry):
        for tap in range(9):
            for a in range(3):
                wc_ref[
                    pl.ds(pl.multiple_of(tap * 128 + n * 16, 16), 16), a * 256 : a * 256 + 256
                ] = wt[n, 9 * a + tap]
        return carry

    lax.fori_loop(0, NT, arrange, 0)

    for part, sem in (
        (a1.at[pl.ds(1, 7)], sa1),
        (b1.at[pl.ds(1, 31)], sb1),
        (lbuf.at[pl.ds(0, 16)], sl),
        (wt.at[pl.ds(0, 3)], sw),
        (wt.at[pl.ds(0, 4)], ss),
        (b2.at[pl.ds(1, 127)], sb2),
    ):
        await_all(part, sem)
    await_all(b2.at[pl.ds(1, 127)], rb2)
    totals = [jnp.sum(b2[64 * s : 64 * s + 64], axis=0) for s in range(2)]
    stats = decode(totals, float(2 * 16 * LCW * TILES * 8))
    for i, s in enumerate((1, 0)):
        alpha = 0.5 * gain2[...] * stats[s][1]
        beta = 0.5 * shift2[...] - stats[s][0] * alpha
        if s == 0:
            params_ref[2:3] = alpha
            params_ref[3:4] = beta
            alpha_before, beta_before = (
                jnp.where(tm == 0, now_, before_) for now_, before_ in ((alpha, last[0]), (beta, last[1]))
            )
            params_ref[0:1] = alpha_before
            params_ref[1:2] = beta_before
        last = alpha, beta


def back_kernel(
    mid, params, inside, blend, wc, out_ref, xs, prod, rows
):
    bias = params[4:5, 0:128]
    for r in range(3):
        for p in range(3):
            for k in range(3):
                values = mid[k * 9 + r * 3 + p]
                keep = inside[k]

                def activate(v, row):
                    half = v * params[row : row + 1] + params[row + 1 : row + 2]
                    return keep * (half + half * jnp.tanh(half))

                before = activate(values[0:16], 0)
                now = activate(values[16:32], 2)
                at = (r * 3 + p) * 48 + k * 16
                xs[at : at + 16, 0:256] = before.astype(BF)
                xs[at : at + 16, 256:512] = jnp.concatenate([before[8:16], now[0:8]], axis=0).astype(BF)
                xs[at : at + 16, 512:768] = now.astype(BF)

    for n in range(0, 9, 2):
        many = min(2, 9 - n)
        result = lax.dot_general(
            xs[...], wc[n * 128 : (n + many) * 128], (((1,), (1,)), ((), ())), preferred_element_type=F32
        )
        for i in range(many):
            prod[n + i] = result[:, i * 128 : i * 128 + 128]

    def products(b, r, at):
        return [
            [prod[3 * b + d, (r * 3 + p) * 48 + at : (r * 3 + p) * 48 + at + 8] for p in range(3)]
            for d in range(3)
        ]

    for t in range(2):
        across = {}
        for k in range(3):
            at = k * 16 + t * 8
            for b in range(3):
                for r in range(3):
                    (a0, a1, a3), (b0, b1, b3), (c0, c1, c3) = products(b, r, at)
                    bc1 = b1 + c1
                    ab1 = a1 + b1
                    across[k, b, r] = (
                        pltpu.roll(a3, 1, 0) + (b0 + c0),
                        (a0 + b0) + c1,
                        a0 + bc1,
                        ab1 + c1,
                        ab1 + c3,
                        a1 + (b3 + c3),
                        (a3 + b3) + pltpu.roll(c0, 7, 0),
                    )
        for c in range(7):
            columns = (3, 4) if c == 3 else (c if c < 3 else c + 1,)
            totals = [[None] * 7 for _ in columns]
            for k in range(3):
                (x0, x1, x3), (y0, y1, y3), (z0, z1, z3) = [
                    [across[k, b, r][c] for r in range(3)] for b in range(3)
                ]
                xy1, yz1 = x1 + y1, y1 + z1
                down = (
                    y0 + z0,
                    (x0 + y0) + z1,
                    x0 + yz1,
                    xy1 + z1,
                    xy1 + z3,
                    x1 + (y3 + z3),
                    x3 + y3,
                )
                for r in range(7):
                    value = (down[r] + bias).astype(BF).astype(F32)
                    for i, column in enumerate(columns):
                        piece = value * blend[3 * column + k]
                        totals[i][r] = piece if k == 0 else totals[i][r] + piece
            for i, column in enumerate(columns):
                for r in range(7):
                    rows[r, pl.ds(column, 8, stride=8), :] = totals[i][r]
        for r in range(7):
            final = rows[r, 8:48].astype(BF)
            for big_row in (3, 4) if r == 3 else (r if r < 3 else r + 1,):
                out_ref[t, big_row] = final


def on_device(
    latent,
    proj_weight,
    first_gain,
    first_shift,
    half_weight,
    second_gain,
    second_shift,
    full_weight,
    full_bias,
    anchors,
    reach,
):
    lat = latent.transpose(1, 2, 3, 0, 4).reshape(LCW, 2, 16)
    shard = full_weight.transpose(0, 2, 1)
    any_space = pl.BlockSpec(memory_space=pl.ANY)
    vmem = pl.BlockSpec(memory_space=pltpu.VMEM)
    dma = pltpu.SemaphoreType.DMA
    held = pl.pallas_call(
        front_kernel,
        name="front",
        out_shape=(
            jax.ShapeDtypeStruct((27, 32, 256), F32),
            jax.ShapeDtypeStruct((8, 256), F32),
            jax.ShapeDtypeStruct((3, 16, 256), F32),
            jax.ShapeDtypeStruct((24, 8, 128), F32),
            jax.ShapeDtypeStruct((9 * 128, 768), BF),
        ),
        in_specs=[any_space] * 11,
        out_specs=(vmem,) * 5,
        scratch_shapes=[
            pltpu.VMEM((3 * (LCW + 2), 2, 16), BF),
            pltpu.VMEM((16, 256), BF),
            pltpu.VMEM((1, 256), F32),
            pltpu.VMEM((1, 256), F32),
            pltpu.VMEM((27, 256, 256), BF),
            pltpu.VMEM((NT, 27, 16, 256), BF),
            pltpu.SMEM((TILES + 1,), jnp.int32),
            pltpu.SMEM((TILES + 1,), jnp.int32),
            pltpu.VMEM((1, 256), F32),
            pltpu.VMEM((1, 256), F32),
            pltpu.VMEM((1, 128), F32),
            pltpu.VMEM((48, 16), F32),
            pltpu.VMEM((256, 128), BF),
            pltpu.VMEM((8, 1, 128), F32),
            pltpu.VMEM((32, 1, 128), F32),
            pltpu.VMEM((128, 1, 128), F32),
            dma((13,)),
            *[dma] * 12,
        ],
        compiler_params=pltpu.CompilerParams(
            collective_id=0, has_side_effects=True, vmem_limit_bytes=20 * 2**20
        ),
    )(
        *(
            pltpu.with_memory_space_constraint(v, pltpu.HBM)
            for v in (
                lat, proj_weight, first_gain.reshape(1, 256), first_shift.reshape(1, 256),
                half_weight, shard, anchors, reach,
                second_gain.reshape(1, 256), second_shift.reshape(1, 256), full_bias.reshape(1, 128),
            )
        )
    )
    out = pl.pallas_call(
        back_kernel,
        name="back",
        out_shape=jax.ShapeDtypeStruct((2, 8, 8 * LCW, 128), BF),
        in_specs=[vmem] * 5,
        out_specs=vmem,
        scratch_shapes=[
            pltpu.VMEM((432, 768), BF),
            pltpu.VMEM((9, 432, 128), F32),
            pltpu.VMEM((7, 64, 128), F32),
        ],
        compiler_params=pltpu.CompilerParams(vmem_limit_bytes=20 * 2**20),
    )(*held)
    return out[:, None]


def solution(mesh):
    return jax.shard_map(
        on_device,
        mesh=mesh,
        in_specs=(
            P("tm", "tile", None, None, None),
            P(),
            P(),
            P(),
            P(),
            P(),
            P(),
            P(None, None, "tm"),
            P(),
            P(),
            P(),
        ),
        out_specs=P("tm", "tile", None, None, None),
        check_vma=False,
    )
```
